256 devices in a mesh: dp: 8 (over y, core), tensor: 4 (over x), ctx: 8 (over z).
Axes of the slice: x: 4, y: 4, z: 8, core: 2. Of those that a mesh axis runs over, the one named last changes fastest.
Arguments:
- grad_down: bfloat16 [8, 18432, 4608], P('dp', 'tensor', 'ctx'), may hold values from -700 to 700
- grad_query: bfloat16 [8, 4608, 2048], P('dp', 'ctx', 'tensor'), may hold values from -700 to 700
- down_param: float32 [18432, 4608], P(('tensor', 'dp'), 'ctx'), may hold values from -0.3 to 0.3
- down_moment: float32 [18432, 4608], P(('tensor', 'dp'), 'ctx'), may hold values from -6 to 6
- down_second: float32 [4608], P('ctx'), may hold values from 0.1 to 2
- query_param: float32 [4608, 2048], P(('ctx', 'dp'), 'tensor'), may hold values from -0.3 to 0.3
- query_moment: float32 [4608, 2048], P(('ctx', 'dp'), 'tensor'), may hold values from -6 to 6
- query_second: float32 [16], P('tensor'), may hold values from 0.1 to 2
- step_count: int32 [1], replicated, may hold values from 1 to 29
Outputs:
- down_param_new: float32 [18432, 4608], P(('tensor', 'dp'), 'ctx')
- down_moment_new: float32 [18432, 4608], P(('tensor', 'dp'), 'ctx')
- down_second_new: float32 [4608], P('ctx')
- down_update: bfloat16 [18432, 4608], P(('tensor', 'dp'), 'ctx')
- query_param_new: float32 [4608, 2048], P(('ctx', 'dp'), 'tensor')
- query_moment_new: float32 [4608, 2048], P(('ctx', 'dp'), 'tensor')
- query_second_new: float32 [16], P('tensor')
- query_update: bfloat16 [4608, 2048], P(('ctx', 'dp'), 'tensor')
The draws below stay inside these ranges and needn't reach their ends.
All inputs are finite; a program needn't handle non-finite values.
Results may differ from the reference program's by a relative error of at most 0.012.
Values may be sent and summed in bfloat16 or wider, within the bound.
No kernel may reach another device: no remote copies, remote signals or barrier semaphores. Data moves between devices by JAX's collectives and lax.ppermute only.
A program may use at most 64 MiB of HBM per device.

```python
import math
import jax
import jax.numpy as jnp
from jax import lax

D = 4608
HEAD_DIM = 128
FF = 18432
HEADS = 16
N_DP = 8


def gradient_field(key, row_count, col_count):
    subkeys = jax.random.split(key, 4)
    row_ramp = jnp.sqrt(3.0) ** (jnp.arange(row_count, dtype=jnp.float32) / row_count)
    row_scale = jnp.exp(jax.random.uniform(subkeys[0], (row_count,), jnp.float32, 0.0, math.log(10.0))) * row_ramp
    col_spread = math.log(10.0)
    col_scale = jnp.exp(jax.random.uniform(subkeys[1], (col_count,), jnp.float32, 0.0, col_spread))
    replica_ramp = jnp.sqrt(3.0) ** (jnp.arange(N_DP, dtype=jnp.float32) / max(N_DP - 1, 1))
    entries = 0.1 * math.sqrt(N_DP) * jax.random.truncated_normal(subkeys[3], -4.0, 4.0, (N_DP, row_count, col_count), jnp.float32)
    return entries * replica_ramp[:, None, None] * row_scale[None, :, None] * col_scale[None, None, :]


def draw_grad_down(key, part):
    return gradient_field(jax.random.fold_in(key, 11), FF, D).astype(jnp.bfloat16)


def draw_grad_query(key, part):
    return gradient_field(jax.random.fold_in(key, 23), D, HEADS * HEAD_DIM).astype(jnp.bfloat16)


def block_levels(key, extent, shards, least, largest):
    def one(axis_at, blocks):
        heights = jax.random.uniform(jax.random.fold_in(jax.random.fold_in(key, 6), axis_at), (blocks,), jnp.float32, least / len(shards), largest / len(shards))
        return jnp.repeat(jnp.exp(heights), extent[axis_at] // blocks).reshape((-1,) + (1,) * (len(extent) - axis_at - 1))

    loudness = one(*shards[0])
    for cut in shards[1:]:
        loudness = loudness * one(*cut)
    return loudness


def gaussian(rng, extent, width, limit, pieces=(), kind=jnp.bfloat16):
    gain = block_levels(rng, extent, pieces, -0.22, 0.18) if pieces else 1.0
    result = jax.random.normal(rng, extent, jnp.float32) * width * gain
    return jnp.minimum(jnp.maximum(result, -limit), limit).astype(kind)


def setup_inputs(seed: int = 0) -> dict:
    keys = jax.random.split(jax.random.key(seed), 10)
    grad_down = draw_grad_down(jax.random.fold_in(keys[9], 71), 0)
    grad_query = draw_grad_query(jax.random.fold_in(keys[9], 71), 0)
    down_param = gaussian(keys[2], (FF, D), 0.05, 0.3, ((0, 32), (1, 8)), jnp.float32)
    down_moment = gaussian(keys[3], (FF, D), 1.0, 6.0, ((0, 32), (1, 8)), jnp.float32)
    down_second = jnp.clip(jnp.exp(math.log(2.0) - 2.9957323 * jax.random.uniform(keys[4], (D,), jnp.float32) ** block_levels(keys[4], (D,), ((0, 8),), -0.2, 0.2)), 0.1, 2.0)
    query_param = gaussian(keys[5], (D, HEADS * HEAD_DIM), 0.05, 0.3, ((0, 64), (1, 4)), jnp.float32)
    query_moment = gaussian(keys[6], (D, HEADS * HEAD_DIM), 1.0, 6.0, ((0, 64), (1, 4)), jnp.float32)
    query_second = jnp.clip(jnp.exp(math.log(2.0) - 2.9957323 * jax.random.uniform(keys[7], (HEADS,), jnp.float32) ** block_levels(keys[7], (HEADS,), ((0, 4),), -0.2, 0.2)), 0.1, 2.0)
    step_count = jax.random.randint(keys[8], (1,), 1, 30).astype(jnp.int32)
    return dict(grad_down=grad_down, grad_query=grad_query, down_param=down_param, down_moment=down_moment, down_second=down_second, query_param=query_param, query_moment=query_moment, query_second=query_second, step_count=step_count)


BETA_ONE = 0.9
BETA_TWO = 0.95
EPSILON = 1e-08
LEARN_RATE = 0.003
DECAY_RATE = 0.1

def replica_mean(gradients):

    def accumulate(position, running_total):
        return running_total + lax.dynamic_index_in_dim(gradients, position, 0, keepdims=False).astype(jnp.float32)
    summed = lax.fori_loop(0, gradients.shape[0], accumulate, jnp.zeros(gradients.shape[1:], jnp.float32))
    return summed / gradients.shape[0]

def finish(parameter, moment, gradient, second_wide, keep_one, keep_two):
    moment_new = BETA_ONE * moment + (1.0 - BETA_ONE) * gradient
    update = moment_new / keep_one / (jnp.sqrt(second_wide / keep_two) + EPSILON)
    parameter_new = parameter - LEARN_RATE * (update + DECAY_RATE * parameter)
    return (parameter_new, moment_new, update.astype(jnp.bfloat16))

def reference(grad_down, grad_query, down_param, down_moment, down_second, query_param, query_moment, query_second, step_count):
    step_value = step_count[0].astype(jnp.float32)
    keep_one = 1.0 - jnp.power(jnp.float32(BETA_ONE), step_value)
    keep_two = 1.0 - jnp.power(jnp.float32(BETA_TWO), step_value)
    down_grad = replica_mean(grad_down)
    query_grad = replica_mean(grad_query)
    neuron_mean = lax.optimization_barrier(jnp.sum(down_grad * down_grad, axis=0)) / FF
    head_mean = lax.optimization_barrier(jnp.sum((query_grad * query_grad).reshape(D, HEADS, HEAD_DIM), axis=(0, 2))) / (D * HEAD_DIM)
    down_second_new = BETA_TWO * down_second + (1.0 - BETA_TWO) * neuron_mean
    query_second_new = BETA_TWO * query_second + (1.0 - BETA_TWO) * head_mean
    down_param_new, down_moment_new, down_update = finish(down_param, down_moment, down_grad, down_second_new[None, :], keep_one, keep_two)
    query_wide = jnp.repeat(query_second_new, HEAD_DIM)
    query_param_new, query_moment_new, query_update = finish(query_param, query_moment, query_grad, query_wide[None, :], keep_one, keep_two)
    return (down_param_new, down_moment_new, down_second_new, down_update, query_param_new, query_moment_new, query_second_new, query_update)
```

```python
import jax
import jax.numpy as jnp
from jax import lax
from jax.experimental import pallas as pl
from jax.experimental.pallas import tpu as pltpu
from jax.sharding import PartitionSpec as P

D = 4608
HEAD_DIM = 128
FF = 18432

BETA_ONE = 0.9
BETA_TWO = 0.95
EPSILON = 1e-08
LEARN_RATE = 0.003
DECAY_RATE = 0.1

LANES = 128
PIECES = ((512, 64), (0, 256), (256, 256))
SLOTS = ((0, 1), (0, 2), (1, 3), (1, 2), (0, 0), (0, 3), (1, 0), (1, 1))
ANY = pl.BlockSpec(memory_space=pl.ANY)
HBM = pl.BlockSpec(memory_space=pltpu.HBM)
VMEM = pl.BlockSpec(memory_space=pltpu.VMEM)
SMEM = pl.BlockSpec(memory_space=pltpu.SMEM)


PARAMS = pltpu.CompilerParams(vmem_limit_bytes=8 << 20)


def pairs(size, mask):
    return [(i, i ^ mask) for i in range(size)]


def far(x):
    return pltpu.with_memory_space_constraint(x, pltpu.HBM)


def near(x):
    return pltpu.with_memory_space_constraint(x, pltpu.VMEM)


def pack_piece(piece, columns, query_chunks, after):
    start, width = PIECES[piece]
    quarter = width // 4
    down_block = 2 * width + quarter
    with_query = piece == 0
    q_rows, q_cols = query_chunks.shape[1:]
    q_wide = q_cols // LANES // 2
    block = down_block + (q_rows * q_wide if with_query else 0)
    total = block * len(SLOTS)
    span = columns.shape[1] // 4

    def kernel(down_ref, query_ref, _, send_ref, own_ref, shared_buf, down_sem, shared_sem, query_sem):
        me = lax.axis_index("dp")
        y, core = me // 2, me % 2
        shared, down, query = [], [], []
        for d in range(4):
            lane = pl.multiple_of(span * (y ^ d) + 4 * LANES, LANES)
            source = down_ref.at[pl.ds(start, width), pl.ds(lane, LANES)]
            shared.append(pltpu.make_async_copy(source, shared_buf.at[d], shared_sem.at[d]))
        for side, out in enumerate((send_ref, own_ref)):
            owner = core if side else 1 - core
            for slot, (half, d) in enumerate(SLOTS):
                for j in range(2):
                    lane = pl.multiple_of(span * (y ^ d) + 5 * LANES * owner + (2 * half + j) * LANES, LANES)
                    source = down_ref.at[pl.ds(start, width), pl.ds(lane, LANES)]
                    target = out.at[pl.ds(slot * block + j * width, width), :]
                    down.append(pltpu.make_async_copy(source, target, down_sem.at[side, slot, j]))
                if with_query:
                    for j in range(q_wide):
                        source = query_ref.at[2 * (y ^ d) + owner, :, pl.ds((half * q_wide + j) * LANES, LANES)]
                        target = out.at[pl.ds(slot * block + down_block + j * q_rows, q_rows), :]
                        query.append(pltpu.make_async_copy(source, target, query_sem.at[side, slot, j]))
        for copy in shared + query + down:
            copy.start()
        for copy in shared:
            copy.wait()
        low = lax.broadcasted_iota(jnp.int32, (quarter, LANES), 1) < LANES // 2
        for slot, (half, d) in enumerate(SLOTS):
            first = shared_buf[d, pl.ds(2 * half * quarter, quarter), :].astype(jnp.float32)
            second = shared_buf[d, pl.ds((2 * half + 1) * quarter, quarter), :].astype(jnp.float32)
            of_core = (
                jnp.where(low, first, pltpu.roll(second, LANES // 2, 1)),
                jnp.where(low, pltpu.roll(first, LANES // 2, 1), second),
            )
            at = (pl.ds(slot * block + 2 * width, quarter), slice(None))
            own_ref[at] = jnp.where(core == 0, of_core[0], of_core[1]).astype(jnp.bfloat16)
            send_ref[at] = jnp.where(core == 0, of_core[1], of_core[0]).astype(jnp.bfloat16)
        for copy in query + down:
            copy.wait()

    shape = pltpu.VMEM((total, LANES), jnp.bfloat16)
    return pl.pallas_call(
        kernel,
        out_shape=(shape, shape),
        in_specs=[HBM, HBM, ANY],
        out_specs=(VMEM, VMEM),
        scratch_shapes=[
            pltpu.VMEM((4, width, LANES), jnp.bfloat16),
            pltpu.SemaphoreType.DMA((2, len(SLOTS), 2)),
            pltpu.SemaphoreType.DMA((4,)),
            pltpu.SemaphoreType.DMA((2, len(SLOTS), q_wide)),
        ],
        compiler_params=PARAMS,
    )(far(columns), far(query_chunks), after)


def added(*terms):
    total = terms[0].astype(jnp.float32)
    for term in terms[1:]:
        total = total + term.astype(jnp.float32)
    return total


def sent(x, mask, axis="dp"):
    return lax.ppermute(x, axis, pairs(8, mask))


def reduce_piece(send, own):
    block = own.shape[0] // len(SLOTS)
    other = sent(send, 1)

    def part(first, count):
        return own[first * block : (first + count) * block], other[first * block : (first + count) * block]

    first_a = sent(added(*part(0, 2)).astype(jnp.bfloat16), 2)
    first_b = sent(added(*part(2, 2)).astype(jnp.bfloat16), 6)
    second_a = sent(added(*part(5, 1), first_a[block:]).astype(jnp.bfloat16), 6)
    second_b = sent(added(*part(7, 1), first_b[block:]).astype(jnp.bfloat16), 2)
    return own, other, first_a, first_b, second_a, second_b


def gather_piece(piece, terms, down_moment, moment_so_far, sums_so_far, query_moment):
    start, width = PIECES[piece]
    quarter = width // 4
    down_block = 2 * width + quarter
    block = terms[0].shape[0] // len(SLOTS)
    first = piece == 0
    q_rows, q_cols = query_moment.shape
    q_wide = q_cols // LANES // 2
    half_tile = LANES // 2

    def kernel(*refs):
        own_ref, other_ref, first_a, first_b, second_a, second_b, moment_ref = refs[:7]
        if first:
            query_moment_ref, new_ref, sums_ref, query_new_ref, query_sums_ref = refs[7:]
            sums_ref[...] = jnp.zeros_like(sums_ref)
            query_sums_ref[...] = jnp.zeros_like(query_sums_ref)
        else:
            _, before_ref, new_ref, sums_ref = refs[7:]
            sums_ref[...] = before_ref[...]
        core = lax.axis_index("dp") % 2

        def mean(half, at, count):
            kept = (4 + 2 * half) * block + at
            step_one, step_two = (first_b, second_b) if half else (first_a, second_a)
            return added(
                own_ref[pl.ds(kept, count), :],
                other_ref[pl.ds(kept, count), :],
                step_one[pl.ds(at, count), :],
                step_two[pl.ds(at, count), :],
            ) * (1.0 / 8.0)

        def column_sum(x):
            return jnp.sum(x * x, axis=0, keepdims=True)

        def moment_new(before, grad):
            return BETA_ONE * before + (1.0 - BETA_ONE) * grad

        step = min(width, LANES)
        for c in range(0, width, step):
            span = slice(start + c, start + c + step)
            total = jnp.zeros((1, step), jnp.float32)
            for tile in range(4):
                half, j = tile // 2, tile % 2
                grad = mean(half, j * width + c, step).T
                at = (pl.ds(pl.multiple_of(half_tile * core + tile * LANES, half_tile), LANES), span)
                new_ref[at] = moment_new(moment_ref[at], grad)
                total += column_sum(grad)
            parts = []
            for part in range(c // quarter, (c + step) // quarter):
                packed = mean(part // 2, 2 * width, quarter)
                parts.append(pltpu.roll(packed, half_tile, 1) if part % 2 else packed)
            grad = jnp.concatenate(parts, axis=0).T[:half_tile]
            at = (pl.ds(pl.multiple_of(4 * LANES * (1 - core), half_tile), half_tile), span)
            new_ref[at] = moment_new(moment_ref[at], grad)
            row = (start + c) // LANES
            sums_ref[row : row + 1, :step] = total + column_sum(grad)
        if first:
            for half in range(2):
                for j in range(q_wide):
                    grad = mean(half, down_block + j * q_rows, q_rows)
                    head = half * q_wide + j
                    at = (slice(None), slice(head * LANES, (head + 1) * LANES))
                    query_new_ref[at] = moment_new(query_moment_ref[at], grad)
                    query_sums_ref[head : head + 1, :] = column_sum(grad)

    new = pltpu.VMEM(down_moment.shape, jnp.float32)
    sums = pltpu.VMEM((8, LANES), jnp.float32)
    terms = tuple(near(t) for t in (*terms, down_moment))
    if first:
        return pl.pallas_call(
            kernel,
            out_shape=(new, sums, pltpu.VMEM(query_moment.shape, jnp.float32), sums),
            in_specs=[VMEM] * 8,
            out_specs=(VMEM,) * 4,
            compiler_params=PARAMS,
        )(*terms, near(query_moment))
    return pl.pallas_call(
        kernel,
        out_shape=(new, sums),
        in_specs=[VMEM] * 9,
        out_specs=(VMEM,) * 2,
        input_output_aliases={7: 0},
        compiler_params=PARAMS,
    )(*terms, near(moment_so_far), near(sums_so_far))


def message_kernel(sums_ref, heads_ref, out_ref, *, tensors):
    me = lax.axis_index("tensor")
    sums = sums_ref[...]
    row = lax.broadcasted_iota(jnp.int32, sums.shape, 0)
    lane = lax.broadcasted_iota(jnp.int32, sums.shape, 1)
    neurons = jnp.where(row < 5, sums, 0.0)
    heads = jnp.sum(heads_ref[...], axis=1, keepdims=True)
    spread = jnp.sum(jnp.where(row == lane, heads, 0.0), axis=0, keepdims=True)
    mine = neurons + jnp.where(row == 5, spread, 0.0)
    for target in range(out_ref.shape[0]):
        out_ref[target] = jnp.where(me == target % tensors, mine, neurons)


ROW_BLOCKS = 6


def finish_kernel(
    keep_ref, got_ref, new_ref, param_ref, second_ref, query_new_ref, query_param_ref, query_second_ref,
    param_out, moment_out, update_out, second_out, query_param_out, query_moment_out, query_update_out, query_second_out,
    param_buf, update_buf, query_param_buf, query_update_buf, sems, query_sems,
):
    keep_one, keep_two = keep_ref[0], keep_ref[1]
    moments = (
        pltpu.make_async_copy(new_ref, moment_out, sems.at[0, 0]),
        pltpu.make_async_copy(query_new_ref, query_moment_out, query_sems.at[0]),
    )
    for copy in moments:
        copy.start()
    total = jnp.sum(got_ref[...], axis=0)

    def second_new(before, mean):
        return BETA_TWO * before + (1.0 - BETA_TWO) * mean

    def factor(second):
        return 1.0 / (keep_one * (jnp.sqrt(second / keep_two) + EPSILON))

    def write(at, scale, new, param, update_to, param_to):
        old = param[at]
        update = new[at] * scale
        update_to[at] = update.astype(jnp.bfloat16)
        param_to[at] = old - LEARN_RATE * (update + DECAY_RATE * old)

    rows, cols = new_ref.shape
    spans = [slice(k, min(k + LANES, cols)) for k in range(0, cols, LANES)]
    factors = []
    for k, span in enumerate(spans):
        second = second_new(second_ref[:, span], total[k : k + 1, : span.stop - span.start] * (1.0 / FF))
        second_out[:, span] = second
        factors.append(factor(second))
    copies = []
    block = rows // ROW_BLOCKS
    for b in range(ROW_BLOCKS):
        part = slice(b * block, (b + 1) * block)
        for span, scale in zip(spans, factors):
            write((part, span), scale, new_ref, param_ref, update_buf, param_buf)
        copies.append(pltpu.make_async_copy(param_buf.at[part], param_out.at[part], sems.at[1, b]))
        copies.append(pltpu.make_async_copy(update_buf.at[part], update_out.at[part], sems.at[2, b]))
        copies[-2].start()
        copies[-1].start()
    heads = query_new_ref.shape[1] // HEAD_DIM
    for head in range(heads):
        mean = total[5:6, head : head + 1] * (1.0 / (D * HEAD_DIM))
        second = second_new(query_second_ref[:, head : head + 1], mean)
        query_second_out[:, head : head + 1] = second
        span = slice(head * HEAD_DIM, (head + 1) * HEAD_DIM)
        write((slice(None), span), factor(second), query_new_ref, query_param_ref, query_update_buf, query_param_buf)
    copies.append(pltpu.make_async_copy(query_param_buf, query_param_out, query_sems.at[1]))
    copies.append(pltpu.make_async_copy(query_update_buf, query_update_out, query_sems.at[2]))
    copies[-2].start()
    copies[-1].start()
    for copy in (*moments, *copies):
        copy.wait()


def shards(
    grad_down,
    grad_query,
    down_param,
    down_moment,
    down_second,
    query_param,
    query_moment,
    query_second,
    step_count,
):
    replicas = lax.axis_size("dp")
    step_value = step_count[0].astype(jnp.float32)
    keep = jnp.stack(
        [1.0 - jnp.power(jnp.float32(BETA_ONE), step_value), 1.0 - jnp.power(jnp.float32(BETA_TWO), step_value)]
    )
    columns = grad_down[0].T
    query_chunks = grad_query[0].reshape(replicas, -1, grad_query.shape[2])
    own, new, sums = query_chunks, None, None
    for piece in range(len(PIECES)):
        send, own = pack_piece(piece, columns, query_chunks, own)
        terms = reduce_piece(send, own)
        result = gather_piece(piece, terms, down_moment, new, sums, query_moment)
        new, sums = result[:2]
        if piece == 0:
            query_new, heads = result[2:]
            for mask in (1, 2, 4):
                heads = heads + sent(heads, mask, "ctx")
    group = ("dp", "tensor")
    tensors = lax.axis_size("tensor")
    message = pl.pallas_call(
        lambda *refs: message_kernel(*refs, tensors=tensors),
        out_shape=pltpu.VMEM((lax.axis_size(group), 8, LANES), jnp.float32),
        in_specs=[VMEM, VMEM],
        out_specs=VMEM,
        compiler_params=PARAMS, name="message",
    )(near(sums), near(heads))
    got = lax.all_to_all(message, group, split_axis=0, concat_axis=0, tiled=True)
    f32, bf16 = jnp.float32, jnp.bfloat16
    outs = pl.pallas_call(
        finish_kernel,
        out_shape=(
            jax.ShapeDtypeStruct(down_param.shape, f32),
            jax.ShapeDtypeStruct(down_param.shape, f32),
            jax.ShapeDtypeStruct(down_param.shape, bf16),
            jax.ShapeDtypeStruct((1, down_param.shape[1]), f32),
            jax.ShapeDtypeStruct(query_param.shape, f32),
            jax.ShapeDtypeStruct(query_param.shape, f32),
            jax.ShapeDtypeStruct(query_param.shape, bf16),
            jax.ShapeDtypeStruct((1, query_second.shape[0]), f32),
        ),
        in_specs=[SMEM] + [VMEM] * 7,
        out_specs=(ANY, ANY, ANY, VMEM, ANY, ANY, ANY, VMEM),
        scratch_shapes=[
            pltpu.VMEM(down_param.shape, f32),
            pltpu.VMEM(down_param.shape, bf16),
            pltpu.VMEM(query_param.shape, f32),
            pltpu.VMEM(query_param.shape, bf16),
            pltpu.SemaphoreType.DMA((3, ROW_BLOCKS)),
            pltpu.SemaphoreType.DMA((3,)),
        ],
        compiler_params=PARAMS, name="finish",
    )(
        keep, near(got), near(new), near(down_param), down_second[None, :],
        near(query_new), near(query_param), query_second[None, :],
    )
    (down_param_new, down_moment_new, down_update, down_second_new) = outs[:4]
    (query_param_new, query_moment_new, query_update, query_second_new) = outs[4:]
    return (
        down_param_new,
        down_moment_new,
        down_second_new[0],
        down_update,
        query_param_new,
        query_moment_new,
        query_second_new[0],
        query_update,
    )


def solution(mesh):
    in_specs = (
        P("dp", "tensor", "ctx"),
        P("dp", "ctx", "tensor"),
        P(("tensor", "dp"), "ctx"),
        P(("tensor", "dp"), "ctx"),
        P("ctx"),
        P(("ctx", "dp"), "tensor"),
        P(("ctx", "dp"), "tensor"),
        P("tensor"),
        P(),
    )
    out_specs = (
        P(("tensor", "dp"), "ctx"),
        P(("tensor", "dp"), "ctx"),
        P("ctx"),
        P(("tensor", "dp"), "ctx"),
        P(("ctx", "dp"), "tensor"),
        P(("ctx", "dp"), "tensor"),
        P("tensor"),
        P(("ctx", "dp"), "tensor"),
    )

    return jax.shard_map(shards, mesh=mesh, in_specs=in_specs, out_specs=out_specs, check_vma=False)
```

```python
import jax
import jax.numpy as jnp
from jax import lax
from jax.experimental import pallas as pl
from jax.experimental.pallas import tpu as pltpu
from jax.sharding import PartitionSpec as P

D = 4608
HEAD_DIM = 128
FF = 18432

BETA_ONE = 0.9
BETA_TWO = 0.95
EPSILON = 1e-08
LEARN_RATE = 0.003
DECAY_RATE = 0.1

LANES = 128
ROW_BLOCKS = 6
PIECES = ((0, 256), (256, 320))
SLOTS = ((0, 1), (0, 2), (1, 3), (1, 2), (0, 0), (0, 3), (1, 0), (1, 1))
ANY = pl.BlockSpec(memory_space=pl.ANY)
HBM = pl.BlockSpec(memory_space=pltpu.HBM)
VMEM = pl.BlockSpec(memory_space=pltpu.VMEM)
SMEM = pl.BlockSpec(memory_space=pltpu.SMEM)


PARAMS = pltpu.CompilerParams(vmem_limit_bytes=8 << 20)


def pairs(size, mask):
    return [(i, i ^ mask) for i in range(size)]


def far(x):
    return pltpu.with_memory_space_constraint(x, pltpu.HBM)


def near(x):
    return pltpu.with_memory_space_constraint(x, pltpu.VMEM)


def down_rows(piece):
    return 2 * PIECES[piece][1] + PIECES[piece][1] // 4


def query_rows(piece, query_chunks):
    return query_chunks.shape[1] * query_chunks.shape[2] // LANES if piece == 0 else 0


def down_at(piece, query, slot):
    return slot * down_rows(piece) + query * (0 if slot < 2 else 1 if slot < 4 else 2)


def query_at(query, d):
    block = down_rows(0)
    return {1: 2 * block, 3: 4 * block + query, 2: 8 * block + 2 * query, 0: 8 * block + 3 * query}[d]


def piece_rows(piece, query):
    return len(SLOTS) * down_rows(piece) + 4 * query


def pack(parts, columns, query_chunks, after):
    q_rows, q_cols = query_chunks.shape[1:]
    heads = q_cols // LANES
    span = columns.shape[1] // 4
    slots = len(SLOTS)

    def kernel(down_ref, query_ref, _, *refs):
        outs, bufs, sems = refs[: len(parts)], refs[len(parts) : 2 * len(parts)], refs[2 * len(parts) :]
        me = lax.axis_index("dp")
        y, core = me // 2, me % 2
        shared, whole = [], []
        for (piece, mine), out, buf, sem in zip(parts, outs, bufs, sems):
            start, width = PIECES[piece]
            query = query_rows(piece, query_chunks)
            owner = core if mine else 1 - core
            for d in range(4):
                lane = pl.multiple_of(span * (y ^ d) + 4 * LANES, LANES)
                source = down_ref.at[pl.ds(start, width), pl.ds(lane, LANES)]
                shared.append(pltpu.make_async_copy(source, buf.at[d], sem.at[slots, d]))
            for slot, (half, d) in enumerate(SLOTS):
                for j in range(2):
                    lane = pl.multiple_of(span * (y ^ d) + 5 * LANES * owner + (2 * half + j) * LANES, LANES)
                    source = down_ref.at[pl.ds(start, width), pl.ds(lane, LANES)]
                    target = out.at[pl.ds(down_at(piece, query, slot) + j * width, width), :]
                    whole.append(pltpu.make_async_copy(source, target, sem.at[slot, j]))
            if piece == 0:
                for d in range(4):
                    for head in range(heads):
                        source = query_ref.at[2 * (y ^ d) + owner, :, pl.ds(head * LANES, LANES)]
                        target = out.at[pl.ds(query_at(query, d) + head * q_rows, q_rows), :]
                        whole.append(pltpu.make_async_copy(source, target, sem.at[2 * d + head // 2, 2 + head % 2]))
        for copy in shared + whole:
            copy.start()
        for copy in shared:
            copy.wait()
        for (piece, mine), out, buf in zip(parts, outs, bufs):
            width = PIECES[piece][1]
            quarter = width // 4
            lower = (core == 0) if mine else (core == 1)
            low = lax.broadcasted_iota(jnp.int32, (quarter, LANES), 1) < LANES // 2
            for slot, (half, d) in enumerate(SLOTS):
                first = buf[d, pl.ds(2 * half * quarter, quarter), :].astype(jnp.float32)
                second = buf[d, pl.ds((2 * half + 1) * quarter, quarter), :].astype(jnp.float32)
                packed = jnp.where(
                    lower,
                    jnp.where(low, first, pltpu.roll(second, LANES // 2, 1)),
                    jnp.where(low, pltpu.roll(first, LANES // 2, 1), second),
                )
                row = down_at(piece, query_rows(piece, query_chunks), slot) + 2 * width
                at = (pl.ds(row, quarter), slice(None))
                out[at] = packed.astype(jnp.bfloat16)
        for copy in whole:
            copy.wait()

    return pl.pallas_call(
        kernel,
        out_shape=tuple(
            pltpu.VMEM((piece_rows(p, query_rows(p, query_chunks)), LANES), jnp.bfloat16) for p, _ in parts
        ),
        in_specs=[HBM, HBM, ANY],
        out_specs=(VMEM,) * len(parts),
        scratch_shapes=[pltpu.VMEM((4, PIECES[p][1], LANES), jnp.bfloat16) for p, _ in parts]
        + [pltpu.SemaphoreType.DMA((slots + 1, 4)) for _ in parts],
        compiler_params=PARAMS,
    )(far(columns), far(query_chunks), after)


def added(*terms):
    total = terms[0].astype(jnp.float32)
    for term in terms[1:]:
        total = total + term.astype(jnp.float32)
    return total


def sent(x, mask, axis="dp"):
    return lax.ppermute(x, axis, pairs(8, mask))


def reduce_piece(piece, query, other, own):
    block = down_rows(piece)

    def part(first, last):
        return own[first:last], other[first:last]

    b_at, kept_at = down_at(piece, query, 2), down_at(piece, query, 4)
    first_a = added(*part(0, b_at)).astype(jnp.bfloat16)
    first_b = added(*part(b_at, kept_at)).astype(jnp.bfloat16)
    if query:
        across = added(*part(query_at(query, 2), query_at(query, 2) + query)).astype(jnp.bfloat16)
    first_a = sent(first_a, 2)
    first_b = sent(first_b, 6)
    if query:
        across = sent(across, 4)
    a_at, b_at = down_at(piece, query, 5), down_at(piece, query, 7)
    second_a = added(*part(a_at, a_at + block), first_a[block : 2 * block]).astype(jnp.bfloat16)
    second_b = added(*part(b_at, b_at + block), first_b[block : 2 * block]).astype(jnp.bfloat16)
    second_a = sent(second_a, 6)
    second_b = sent(second_b, 2)
    return (own, other, first_a, first_b, second_a, second_b), (across if query else None)


def moment_new(before, grad):
    return BETA_ONE * before + (1.0 - BETA_ONE) * grad


def column_sum(x):
    return jnp.sum(x * x, axis=0, keepdims=True)


def gather_query(query, terms, across, query_moment):
    q_rows, q_cols = query_moment.shape
    block = down_rows(0)

    def kernel(own_ref, other_ref, first_a, first_b, across_ref, moment_ref, new_ref, sums_ref):
        sums_ref[...] = jnp.zeros_like(sums_ref)
        for head in range(q_cols // LANES):
            at = head * q_rows
            grad = added(
                own_ref[pl.ds(query_at(query, 0) + at, q_rows), :],
                other_ref[pl.ds(query_at(query, 0) + at, q_rows), :],
                first_a[pl.ds(2 * block + at, q_rows), :],
                first_b[pl.ds(2 * block + at, q_rows), :],
                across_ref[pl.ds(at, q_rows), :],
            ) * (1.0 / 8.0)
            span = (slice(None), slice(head * LANES, (head + 1) * LANES))
            new_ref[span] = moment_new(moment_ref[span], grad)
            sums_ref[head : head + 1, :] = column_sum(grad)

    return pl.pallas_call(
        kernel,
        out_shape=(pltpu.VMEM(query_moment.shape, jnp.float32), pltpu.VMEM((8, LANES), jnp.float32)),
        in_specs=[VMEM] * 6,
        out_specs=(VMEM,) * 2,
        compiler_params=PARAMS,
        name="query",
    )(*(near(t) for t in (*terms[:4], across, query_moment)))


def gather_piece(piece, query, terms, down_moment, so_far):
    start, width = PIECES[piece]
    quarter = width // 4
    first, last = piece == 0, piece == len(PIECES) - 1
    half_tile = LANES // 2
    tensors = lax.axis_size("tensor")

    def kernel(*refs):
        own_ref, other_ref, first_a, first_b, second_a, second_b, moment_ref = refs[:7]
        if first:
            new_ref, sums_ref = refs[7:]
            sums_ref[...] = jnp.zeros_like(sums_ref)
        elif last:
            _, before_ref, heads_ref, new_ref, message_ref, sums_ref = refs[7:]
            sums_ref[...] = before_ref[...]
        else:
            _, before_ref, new_ref, sums_ref = refs[7:]
            sums_ref[...] = before_ref[...]
        core = lax.axis_index("dp") % 2

        def mean(half, at, count):
            kept = down_at(piece, query, 4 + 2 * half) + at
            step_one, step_two = (first_b, second_b) if half else (first_a, second_a)
            return added(
                own_ref[pl.ds(kept, count), :],
                other_ref[pl.ds(kept, count), :],
                step_one[pl.ds(at, count), :],
                step_two[pl.ds(at, count), :],
            ) * (1.0 / 8.0)

        parts = []
        for part in range(4):
            packed = mean(part // 2, 2 * width, quarter)
            parts.append(pltpu.roll(packed, half_tile, 1) if part % 2 else packed)
        rest = jnp.concatenate(parts, axis=0)
        for c in range(0, width, LANES):
            step = min(LANES, width - c)
            span = slice(start + c, start + c + step)
            total = jnp.zeros((1, step), jnp.float32)
            for tile in range(4):
                half, j = tile // 2, tile % 2
                grad = mean(half, j * width + c, step).T
                at = (pl.ds(pl.multiple_of(half_tile * core + tile * LANES, half_tile), LANES), span)
                new_ref[at] = moment_new(moment_ref[at], grad)
                total += column_sum(grad)
            grad = rest[c : c + step].T[:half_tile]
            at = (pl.ds(pl.multiple_of(4 * LANES * (1 - core), half_tile), half_tile), span)
            new_ref[at] = moment_new(moment_ref[at], grad)
            row = (start + c) // LANES
            sums_ref[row : row + 1, :step] = total + column_sum(grad)
        if last:
            me = lax.axis_index("tensor")
            sums = sums_ref[...]
            row = lax.broadcasted_iota(jnp.int32, sums.shape, 0)
            lane = lax.broadcasted_iota(jnp.int32, sums.shape, 1)
            neurons = jnp.where(row < 5, sums, 0.0)
            heads = jnp.sum(heads_ref[...], axis=1, keepdims=True)
            spread = jnp.sum(jnp.where(row == lane, heads, 0.0), axis=0, keepdims=True)
            mine = neurons + jnp.where(row == 5, spread, 0.0)
            for target in range(message_ref.shape[0]):
                message_ref[target] = jnp.where(me == target % tensors, mine, neurons)

    new = pltpu.VMEM(down_moment.shape, jnp.float32)
    sums = pltpu.VMEM((8, LANES), jnp.float32)
    out_shape, extra = (new, sums), so_far
    scratch = []
    if last:
        message = pltpu.VMEM((lax.axis_size("dp") * tensors, 8, LANES), jnp.float32)
        out_shape, scratch = (new, message), [sums]
    operands = tuple(near(t) for t in (*terms, down_moment, *extra))
    return pl.pallas_call(
        kernel,
        out_shape=out_shape,
        in_specs=[VMEM] * len(operands),
        out_specs=(VMEM,) * len(out_shape),
        scratch_shapes=scratch,
        input_output_aliases={} if first else {7: 0},
        compiler_params=PARAMS,
    )(*operands)


def store_kernel(new_ref, query_new_ref, moment_out, query_moment_out, sems):
    copies = (
        pltpu.make_async_copy(new_ref, moment_out, sems.at[0]),
        pltpu.make_async_copy(query_new_ref, query_moment_out, sems.at[1]),
    )
    for copy in copies:
        copy.start()
    for copy in copies:
        copy.wait()


def finish_kernel(
    keep_ref, got_ref, new_ref, param_ref, second_ref, query_new_ref, query_param_ref, query_second_ref,
    param_out, update_out, second_out, query_param_out, query_update_out, query_second_out,
    param_buf, update_buf, query_param_buf, query_update_buf, sems, query_sems,
):
    keep_one, keep_two = keep_ref[0], keep_ref[1]
    total = jnp.sum(got_ref[...], axis=0)

    def second_new(before, mean):
        return BETA_TWO * before + (1.0 - BETA_TWO) * mean

    def factor(second):
        return 1.0 / (keep_one * (jnp.sqrt(second / keep_two) + EPSILON))

    def write(at, scale, new, param, update_to, param_to):
        old = param[at]
        update = new[at] * scale
        update_to[at] = update.astype(jnp.bfloat16)
        param_to[at] = old - LEARN_RATE * (update + DECAY_RATE * old)

    rows, cols = new_ref.shape
    spans = [slice(k, min(k + LANES, cols)) for k in range(0, cols, LANES)]
    factors = []
    for k, span in enumerate(spans):
        second = second_new(second_ref[:, span], total[k : k + 1, : span.stop - span.start] * (1.0 / FF))
        second_out[span] = second[0]
        factors.append(factor(second))
    copies = []
    block = rows // ROW_BLOCKS
    for b in range(ROW_BLOCKS):
        part = slice(b * block, (b + 1) * block)
        for span, scale in zip(spans, factors):
            write((part, span), scale, new_ref, param_ref, update_buf, param_buf)
        copies.append(pltpu.make_async_copy(param_buf.at[part], param_out.at[part], sems.at[0, b]))
        copies.append(pltpu.make_async_copy(update_buf.at[part], update_out.at[part], sems.at[1, b]))
        copies[-2].start()
        copies[-1].start()
    heads = query_new_ref.shape[1] // HEAD_DIM
    for head in range(heads):
        mean = total[5:6, head : head + 1] * (1.0 / (D * HEAD_DIM))
        second = second_new(query_second_ref[:, head : head + 1], mean)
        query_second_out[:, head : head + 1] = second
        span = slice(head * HEAD_DIM, (head + 1) * HEAD_DIM)
        write((slice(None), span), factor(second), query_new_ref, query_param_ref, query_update_buf, query_param_buf)
    copies.append(pltpu.make_async_copy(query_param_buf, query_param_out, query_sems.at[0]))
    copies.append(pltpu.make_async_copy(query_update_buf, query_update_out, query_sems.at[1]))
    copies[-2].start()
    copies[-1].start()
    for copy in copies:
        copy.wait()


def shards(
    grad_down,
    grad_query,
    down_param,
    down_moment,
    down_second,
    query_param,
    query_moment,
    query_second,
    step_count,
):
    replicas = lax.axis_size("dp")
    step_value = step_count[0].astype(jnp.float32)
    keep = jnp.stack(
        [1.0 - jnp.power(jnp.float32(BETA_ONE), step_value), 1.0 - jnp.power(jnp.float32(BETA_TWO), step_value)]
    )
    columns = grad_down[0].T
    query_chunks = grad_query[0].reshape(replicas, -1, grad_query.shape[2])
    last = len(PIECES) - 1
    (send,) = pack(((0, False),), columns, query_chunks, query_chunks)
    others, owns = [sent(send, 1)], []
    for piece in range(last):
        own, send = pack(((piece, True), (piece + 1, False)), columns, query_chunks, send)
        owns.append(own)
        others.append(sent(send, 1))
    owns += pack(((last, True),), columns, query_chunks, send)
    so_far = ()
    gathered = []
    for piece in range(len(PIECES)):
        query = query_rows(piece, query_chunks)
        terms, across = reduce_piece(piece, query, others[piece], owns[piece])
        gathered.append((piece, query, terms))
        if query:
            query_new, heads = gather_query(query, terms, across, query_moment)
    for mask in (1, 2, 7):
        heads = heads + sent(heads, mask, "ctx")
    for piece, query, terms in gathered:
        if piece == last:
            so_far += (heads,)
        so_far = gather_piece(piece, query, terms, down_moment, so_far)
    new, message = so_far
    got = lax.all_to_all(message, ("dp", "tensor"), split_axis=0, concat_axis=0, tiled=True)
    down_moment_new, query_moment_new = pl.pallas_call(
        store_kernel,
        out_shape=tuple(pltpu.HBM(x.shape, jnp.float32) for x in (new, query_new)),
        in_specs=[VMEM, VMEM],
        out_specs=(HBM, HBM),
        scratch_shapes=[pltpu.SemaphoreType.DMA((2,))],
        compiler_params=PARAMS,
        name="store",
    )(near(new), near(query_new))
    f32, bf16 = jnp.float32, jnp.bfloat16
    outs = pl.pallas_call(
        finish_kernel,
        out_shape=(
            pltpu.HBM(down_param.shape, f32),
            pltpu.HBM(down_param.shape, bf16),
            jax.ShapeDtypeStruct(down_second.shape, f32),
            pltpu.HBM(query_param.shape, f32),
            pltpu.HBM(query_param.shape, bf16),
            jax.ShapeDtypeStruct((1, query_second.shape[0]), f32),
        ),
        in_specs=[SMEM] + [VMEM] * 7,
        out_specs=(HBM, HBM, VMEM, HBM, HBM, VMEM),
        scratch_shapes=[
            pltpu.VMEM(down_param.shape, f32),
            pltpu.VMEM(down_param.shape, bf16),
            pltpu.VMEM(query_param.shape, f32),
            pltpu.VMEM(query_param.shape, bf16),
            pltpu.SemaphoreType.DMA((2, ROW_BLOCKS)),
            pltpu.SemaphoreType.DMA((2,)),
        ],
        compiler_params=PARAMS, name="finish",
    )(
        keep, near(got), near(new), near(down_param), down_second[None, :],
        near(query_new), near(query_param), query_second[None, :],
    )
    down_param_new, down_update, down_second_new = outs[:3]
    query_param_new, query_update, query_second_new = outs[3:]
    return (
        down_param_new,
        down_moment_new,
        down_second_new,
        down_update,
        query_param_new,
        query_moment_new,
        query_second_new[0],
        query_update,
    )


def solution(mesh):
    in_specs = (
        P("dp", "tensor", "ctx"),
        P("dp", "ctx", "tensor"),
        P(("tensor", "dp"), "ctx"),
        P(("tensor", "dp"), "ctx"),
        P("ctx"),
        P(("ctx", "dp"), "tensor"),
        P(("ctx", "dp"), "tensor"),
        P("tensor"),
        P(),
    )
    out_specs = (
        P(("tensor", "dp"), "ctx"),
        P(("tensor", "dp"), "ctx"),
        P("ctx"),
        P(("tensor", "dp"), "ctx"),
        P(("ctx", "dp"), "tensor"),
        P(("ctx", "dp"), "tensor"),
        P("tensor"),
        P(("ctx", "dp"), "tensor"),
    )

    return jax.shard_map(shards, mesh=mesh, in_specs=in_specs, out_specs=out_specs, check_vma=False)
```

```python
import jax
import jax.numpy as jnp
from jax import lax
from jax.experimental import pallas as pl
from jax.experimental.pallas import tpu as pltpu
from jax.sharding import PartitionSpec as P

D = 4608
HEAD_DIM = 128
FF = 18432

BETA_ONE = 0.9
BETA_TWO = 0.95
EPSILON = 1e-08
LEARN_RATE = 0.003
DECAY_RATE = 0.1

LANES = 128
ROW_BLOCKS = 6
PIECES = ((0, 256), (256, 320))
SLOTS = ((0, 1), (0, 2), (1, 3), (1, 2), (0, 0), (0, 3), (1, 0), (1, 1))
ANY = pl.BlockSpec(memory_space=pl.ANY)
HBM = pl.BlockSpec(memory_space=pltpu.HBM)
VMEM = pl.BlockSpec(memory_space=pltpu.VMEM)


PARAMS = pltpu.CompilerParams(vmem_limit_bytes=8 << 20)


def pairs(size, mask):
    return [(i, i ^ mask) for i in range(size)]


def far(x):
    return pltpu.with_memory_space_constraint(x, pltpu.HBM)


def near(x):
    return pltpu.with_memory_space_constraint(x, pltpu.VMEM)


def down_rows(piece):
    return 2 * PIECES[piece][1] + PIECES[piece][1] // 4


def query_rows(piece, query_chunks):
    return query_chunks.shape[1] * query_chunks.shape[2] // LANES if piece == 0 else 0


def down_at(piece, query, slot):
    return slot * down_rows(piece) + query * (0 if slot < 2 else 1 if slot < 4 else 3)


def query_at(query, d):
    block = down_rows(0)
    return {1: 2 * block, 3: 4 * block + query, 2: 4 * block + 2 * query, 0: 8 * block + 3 * query}[d]


def piece_rows(piece, query):
    return len(SLOTS) * down_rows(piece) + 4 * query


def group(piece, query, part):
    a, b, kept = (down_at(piece, query, slot) for slot in (0, 2, 4))
    end = piece_rows(piece, query)
    return {
        "a": (a, b - a, (0, 1), (1,)),
        "b": (b, kept - b, (2, 3), (3, 2)),
        "kept": (kept, end - kept, (4, 5, 6, 7), (0,)),
        "all": (0, end, tuple(range(len(SLOTS))), (1, 3, 2, 0)),
    }[part]


def pack(parts, columns, query_chunks, after, place):
    q_rows, q_cols = query_chunks.shape[1:]
    heads = q_cols // LANES
    span = columns.shape[1] // 4
    slots = len(SLOTS)

    def kernel(down_ref, query_ref, _, *refs):
        outs, bufs, sems = refs[: len(parts)], refs[len(parts) : 2 * len(parts)], refs[2 * len(parts) :]
        me = lax.axis_index("dp")
        y, core = me // 2, me % 2
        shared, whole = [], []

        def put(copies, source, target, semaphore):
            if place is far:
                copies.append(pltpu.make_async_copy(source, target, semaphore))
            else:
                target[...] = source[...]

        for (piece, part, mine), out, buf, sem in zip(parts, outs, bufs, sems):
            start, width = PIECES[piece]
            query = query_rows(piece, query_chunks)
            base, _, its_slots, its_chunks = group(piece, query, part)
            owner = core if mine else 1 - core
            for d in sorted({SLOTS[slot][1] for slot in its_slots}):
                lane = pl.multiple_of(span * (y ^ d) + 4 * LANES, LANES)
                source = down_ref.at[pl.ds(start, width), pl.ds(lane, LANES)]
                put(shared, source, buf.at[d], sem.at[slots, d])
            for slot in its_slots:
                half, d = SLOTS[slot]
                for j in range(2):
                    lane = pl.multiple_of(span * (y ^ d) + 5 * LANES * owner + (2 * half + j) * LANES, LANES)
                    source = down_ref.at[pl.ds(start, width), pl.ds(lane, LANES)]
                    target = out.at[pl.ds(down_at(piece, query, slot) - base + j * width, width), :]
                    put(whole, source, target, sem.at[slot, j])
            if piece == 0:
                for d in its_chunks:
                    for head in range(heads):
                        source = query_ref.at[2 * (y ^ d) + owner, :, pl.ds(head * LANES, LANES)]
                        target = out.at[pl.ds(query_at(query, d) - base + head * q_rows, q_rows), :]
                        put(whole, source, target, sem.at[2 * d + head // 2, 2 + head % 2])
        for copy in shared + whole:
            copy.start()
        for copy in shared:
            copy.wait()
        for (piece, part, mine), out, buf in zip(parts, outs, bufs):
            width = PIECES[piece][1]
            query = query_rows(piece, query_chunks)
            base, _, its_slots, _ = group(piece, query, part)
            quarter = width // 4
            lower = (core == 0) if mine else (core == 1)
            low = lax.broadcasted_iota(jnp.int32, (quarter, LANES), 1) < LANES // 2
            for slot in its_slots:
                half, d = SLOTS[slot]
                first = buf[d, pl.ds(2 * half * quarter, quarter), :].astype(jnp.float32)
                second = buf[d, pl.ds((2 * half + 1) * quarter, quarter), :].astype(jnp.float32)
                packed = jnp.where(
                    lower,
                    jnp.where(low, first, pltpu.roll(second, LANES // 2, 1)),
                    jnp.where(low, pltpu.roll(first, LANES // 2, 1), second),
                )
                row = down_at(piece, query, slot) - base + 2 * width
                at = (pl.ds(row, quarter), slice(None))
                out[at] = packed.astype(jnp.bfloat16)
        for copy in whole:
            copy.wait()

    return pl.pallas_call(
        kernel,
        out_shape=tuple(
            pltpu.VMEM((group(p, query_rows(p, query_chunks), part)[1], LANES), jnp.bfloat16) for p, part, _ in parts
        ),
        in_specs=[HBM, HBM, ANY] if place is far else [VMEM, VMEM, ANY],
        out_specs=(VMEM,) * len(parts),
        scratch_shapes=[pltpu.VMEM((4, PIECES[p][1], LANES), jnp.bfloat16) for p, _, _ in parts]
        + [pltpu.SemaphoreType.DMA((slots + 1, 4)) for _ in parts],
        compiler_params=PARAMS,
    )(place(columns), place(query_chunks), after)


def added(*terms):
    total = terms[0].astype(jnp.float32)
    for term in terms[1:]:
        total = total + term.astype(jnp.float32)
    return total


def sent(x, mask, axis="dp"):
    return lax.ppermute(x, axis, pairs(8, mask))


def reduce_piece(piece, query, other, own):
    block = down_rows(piece)

    def rows(first, count):
        found = []
        for side in (own, other):
            for part, array in side.items():
                base, size = group(piece, query, part)[:2]
                if base <= first and first + count <= base + size:
                    found.append(array[first - base : first - base + count])
        return found

    b_at = down_at(piece, query, 2)
    first_a = added(*rows(0, b_at)).astype(jnp.bfloat16)
    first_b = added(*rows(b_at, 2 * block + query)).astype(jnp.bfloat16)
    first_a = sent(first_a, 2)
    first_b = sent(first_b, 6)
    across = None
    if query:
        across = added(*rows(query_at(query, 2), query)).astype(jnp.bfloat16)
        across = sent(across, 4)
    a_at, b_at = down_at(piece, query, 5), down_at(piece, query, 7)
    second_a = added(*rows(a_at, block), first_a[block : 2 * block]).astype(jnp.bfloat16)
    second_b = added(*rows(b_at, block), first_b[block : 2 * block]).astype(jnp.bfloat16)
    second_a = sent(second_a, 6)
    second_b = sent(second_b, 2)
    part = "kept" if "kept" in own else "all"
    return (own[part], other[part], first_a, first_b, second_a, second_b), across


def moment_new(before, grad):
    return BETA_ONE * before + (1.0 - BETA_ONE) * grad


def column_sum(x):
    return jnp.sum(x * x, axis=0, keepdims=True)


def gather_query(query, terms, across, query_moment):
    q_rows, q_cols = query_moment.shape
    block = down_rows(0)
    kept = query_at(query, 0) - group(0, query, "kept")[0]

    def kernel(own_ref, other_ref, first_a, first_b, across_ref, moment_ref, new_ref, sums_ref):
        sums_ref[...] = jnp.zeros_like(sums_ref)
        for head in range(q_cols // LANES):
            at = head * q_rows
            grad = added(
                own_ref[pl.ds(kept + at, q_rows), :],
                other_ref[pl.ds(kept + at, q_rows), :],
                first_a[pl.ds(2 * block + at, q_rows), :],
                first_b[pl.ds(2 * block + at, q_rows), :],
                across_ref[pl.ds(at, q_rows), :],
            ) * (1.0 / 8.0)
            span = (slice(None), slice(head * LANES, (head + 1) * LANES))
            new_ref[span] = moment_new(moment_ref[span], grad)
            sums_ref[head : head + 1, :] = column_sum(grad)

    return pl.pallas_call(
        kernel,
        out_shape=(pltpu.VMEM(query_moment.shape, jnp.float32), pltpu.VMEM((8, LANES), jnp.float32)),
        in_specs=[VMEM] * 6,
        out_specs=(VMEM,) * 2,
        compiler_params=PARAMS,
        name="query",
    )(*(near(t) for t in (*terms[:4], across, query_moment)))


def gather_piece(piece, query, terms, down_moment, so_far):
    start, width = PIECES[piece]
    quarter = width // 4
    first, last = piece == 0, piece == len(PIECES) - 1
    base = down_at(piece, query, 4) if first else 0
    half_tile = LANES // 2
    tensors = lax.axis_size("tensor")

    def kernel(*refs):
        own_ref, other_ref, first_a, first_b, second_a, second_b, moment_ref = refs[:7]
        if first:
            new_ref, sums_ref = refs[7:]
            sums_ref[...] = jnp.zeros_like(sums_ref)
        elif last:
            _, before_ref, heads_ref, new_ref, message_ref, sums_ref = refs[7:]
            sums_ref[...] = before_ref[...]
        else:
            _, before_ref, new_ref, sums_ref = refs[7:]
            sums_ref[...] = before_ref[...]
        core = lax.axis_index("dp") % 2

        def mean(half, at, count):
            kept = down_at(piece, query, 4 + 2 * half) - base + at
            step_one, step_two = (first_b, second_b) if half else (first_a, second_a)
            return added(
                own_ref[pl.ds(kept, count), :],
                other_ref[pl.ds(kept, count), :],
                step_one[pl.ds(at, count), :],
                step_two[pl.ds(at, count), :],
            ) * (1.0 / 8.0)

        parts = []
        for part in range(4):
            packed = mean(part // 2, 2 * width, quarter)
            parts.append(pltpu.roll(packed, half_tile, 1) if part % 2 else packed)
        rest = jnp.concatenate(parts, axis=0)
        for c in range(0, width, LANES):
            step = min(LANES, width - c)
            span = slice(start + c, start + c + step)
            total = jnp.zeros((1, step), jnp.float32)
            for tile in range(4):
                half, j = tile // 2, tile % 2
                grad = mean(half, j * width + c, step).T
                at = (pl.ds(pl.multiple_of(half_tile * core + tile * LANES, half_tile), LANES), span)
                new_ref[at] = moment_new(moment_ref[at], grad)
                total += column_sum(grad)
            grad = rest[c : c + step].T[:half_tile]
            at = (pl.ds(pl.multiple_of(4 * LANES * (1 - core), half_tile), half_tile), span)
            new_ref[at] = moment_new(moment_ref[at], grad)
            row = (start + c) // LANES
            sums_ref[row : row + 1, :step] = total + column_sum(grad)
        if last:
            me = lax.axis_index("tensor")
            sums = sums_ref[...]
            row = lax.broadcasted_iota(jnp.int32, sums.shape, 0)
            lane = lax.broadcasted_iota(jnp.int32, sums.shape, 1)
            neurons = jnp.where(row < 5, sums, 0.0)
            heads = jnp.sum(heads_ref[...], axis=1, keepdims=True)
            spread = jnp.sum(jnp.where(row == lane, heads, 0.0), axis=0, keepdims=True)
            mine = neurons + jnp.where(row == 5, spread, 0.0)
            for target in range(message_ref.shape[0]):
                message_ref[target] = jnp.where(me == target % tensors, mine, neurons)

    new = pltpu.VMEM(down_moment.shape, jnp.float32)
    sums = pltpu.VMEM((8, LANES), jnp.float32)
    out_shape, extra = (new, sums), so_far
    scratch = []
    if last:
        message = pltpu.VMEM((lax.axis_size("dp") * tensors, 8, LANES), jnp.float32)
        out_shape, scratch = (new, message), [sums]
    operands = tuple(near(t) for t in (*terms, down_moment, *extra))
    return pl.pallas_call(
        kernel,
        out_shape=out_shape,
        in_specs=[VMEM] * len(operands),
        out_specs=(VMEM,) * len(out_shape),
        scratch_shapes=scratch,
        input_output_aliases={} if first else {7: 0},
        compiler_params=PARAMS,
    )(*operands)


def store_kernel(new_ref, query_new_ref, moment_out, query_moment_out, sems):
    copies = (
        pltpu.make_async_copy(new_ref, moment_out, sems.at[0]),
        pltpu.make_async_copy(query_new_ref, query_moment_out, sems.at[1]),
    )
    for copy in copies:
        copy.start()
    for copy in copies:
        copy.wait()


def finish_kernel(
    keep_ref, got_ref, new_ref, param_ref, second_ref, query_new_ref, query_param_ref, query_second_ref,
    param_out, update_out, second_out, query_param_out, query_update_out, query_second_out,
    param_buf, update_buf, second_buf, query_param_buf, query_update_buf, query_second_buf, sems, query_sems, second_sems,
):
    keep_one, keep_two = keep_ref[:, 0:1], keep_ref[:, 1:2]
    total = jnp.sum(got_ref[...], axis=0)

    def second_new(before, mean):
        return BETA_TWO * before + (1.0 - BETA_TWO) * mean

    def factor(second):
        return 1.0 / (keep_one * (jnp.sqrt(second / keep_two) + EPSILON))

    def write(at, scale, new, param, update_to, param_to):
        old = param[at]
        update = new[at] * scale
        update_to[at] = update.astype(jnp.bfloat16)
        param_to[at] = old - LEARN_RATE * (update + DECAY_RATE * old)

    rows, cols = new_ref.shape
    spans = [slice(k, min(k + LANES, cols)) for k in range(0, cols, LANES)]
    factors = []
    for k, span in enumerate(spans):
        second = second_new(second_ref[:, span], total[k : k + 1, : span.stop - span.start] * (1.0 / FF))
        second_buf[span] = second[0]
        factors.append(factor(second))
    copies = [pltpu.make_async_copy(second_buf, second_out, second_sems.at[0])]
    copies[-1].start()
    block = rows // ROW_BLOCKS
    for b in range(ROW_BLOCKS):
        part = slice(b * block, (b + 1) * block)
        for span, scale in zip(spans, factors):
            write((part, span), scale, new_ref, param_ref, update_buf, param_buf)
        copies.append(pltpu.make_async_copy(param_buf.at[part], param_out.at[part], sems.at[0, b]))
        copies.append(pltpu.make_async_copy(update_buf.at[part], update_out.at[part], sems.at[1, b]))
        copies[-2].start()
        copies[-1].start()
    heads = query_new_ref.shape[1] // HEAD_DIM
    for head in range(heads):
        mean = total[5:6, head : head + 1] * (1.0 / (D * HEAD_DIM))
        second = second_new(query_second_ref[:, head : head + 1], mean)
        query_second_buf[:, head : head + 1] = second
        span = slice(head * HEAD_DIM, (head + 1) * HEAD_DIM)
        write((slice(None), span), factor(second), query_new_ref, query_param_ref, query_update_buf, query_param_buf)
    copies.append(pltpu.make_async_copy(query_param_buf, query_param_out, query_sems.at[0]))
    copies.append(pltpu.make_async_copy(query_update_buf, query_update_out, query_sems.at[1]))
    copies.append(pltpu.make_async_copy(query_second_buf, query_second_out, second_sems.at[1]))
    for copy in copies[-3:]:
        copy.start()
    for copy in copies:
        copy.wait()


def shards(
    grad_down,
    grad_query,
    down_param,
    down_moment,
    down_second,
    query_param,
    query_moment,
    query_second,
    step_count,
):
    replicas = lax.axis_size("dp")
    step_value = step_count[0].astype(jnp.float32)
    keep = jnp.stack(
        [1.0 - jnp.power(jnp.float32(BETA_ONE), step_value), 1.0 - jnp.power(jnp.float32(BETA_TWO), step_value)]
    )
    columns = grad_down[0].T
    query_chunks = grad_query[0].reshape(replicas, -1, grad_query.shape[2])
    last = len(PIECES) - 1
    last = len(PIECES) - 1

    def packed(step, *parts):
        return pack(parts, columns, query_chunks, send, near if step else far)

    send = query_chunks
    send_a, send_b = packed(0, (0, "a", False), (0, "b", False))
    others = [{"a": sent(send_a, 1), "b": sent(send_b, 1)}, {}]
    send = send_a
    own_a, own_b = packed(1, (0, "a", True), (0, "b", True))
    owns = [{"a": own_a, "b": own_b}, {}]
    send = own_a
    (send,) = packed(2, (1, "all", False))
    others[1]["all"] = sent(send, 1)
    owns[0]["kept"], send = packed(3, (0, "kept", True), (0, "kept", False))
    others[0]["kept"] = sent(send, 1)
    (owns[1]["all"],) = packed(4, (1, "all", True))
    so_far = ()
    gathered = []
    for piece in range(len(PIECES)):
        query = query_rows(piece, query_chunks)
        terms, across = reduce_piece(piece, query, others[piece], owns[piece])
        gathered.append((piece, query, terms))
        if query:
            query_new, heads = gather_query(query, terms, across, query_moment)
    for mask in (1, 2, 7):
        heads = heads + sent(heads, mask, "ctx")
    for piece, query, terms in gathered:
        if piece == last:
            so_far += (heads,)
        so_far = gather_piece(piece, query, terms, down_moment, so_far)
    new, message = so_far
    got = lax.all_to_all(message, ("dp", "tensor"), split_axis=0, concat_axis=0, tiled=True)
    down_moment_new, query_moment_new = pl.pallas_call(
        store_kernel,
        out_shape=tuple(pltpu.HBM(x.shape, jnp.float32) for x in (new, query_new)),
        in_specs=[VMEM, VMEM],
        out_specs=(HBM, HBM),
        scratch_shapes=[pltpu.SemaphoreType.DMA((2,))],
        compiler_params=PARAMS,
        name="store",
    )(near(new), near(query_new))
    f32, bf16 = jnp.float32, jnp.bfloat16
    outs = pl.pallas_call(
        finish_kernel,
        out_shape=(
            pltpu.HBM(down_param.shape, f32),
            pltpu.HBM(down_param.shape, bf16),
            pltpu.HBM(down_second.shape, f32),
            pltpu.HBM(query_param.shape, f32),
            pltpu.HBM(query_param.shape, bf16),
            pltpu.HBM((1, query_second.shape[0]), f32),
        ),
        in_specs=[VMEM] * 8,
        out_specs=(HBM,) * 6,
        scratch_shapes=[
            pltpu.VMEM(down_param.shape, f32),
            pltpu.VMEM(down_param.shape, bf16),
            pltpu.VMEM(down_second.shape, f32),
            pltpu.VMEM(query_param.shape, f32),
            pltpu.VMEM(query_param.shape, bf16),
            pltpu.VMEM((1, query_second.shape[0]), f32),
            pltpu.SemaphoreType.DMA((2, ROW_BLOCKS)),
            pltpu.SemaphoreType.DMA((2,)),
            pltpu.SemaphoreType.DMA((2,)),
        ],
        compiler_params=PARAMS, name="finish",
    )(
        near(keep[None, :]), near(got), near(new), near(down_param), near(down_second[None, :]),
        near(query_new), near(query_param), near(query_second[None, :]),
    )
    down_param_new, down_update, down_second_new = outs[:3]
    query_param_new, query_update, query_second_new = outs[3:]
    return (
        down_param_new,
        down_moment_new,
        down_second_new,
        down_update,
        query_param_new,
        query_moment_new,
        query_second_new[0],
        query_update,
    )


def solution(mesh):
    in_specs = (
        P("dp", "tensor", "ctx"),
        P("dp", "ctx", "tensor"),
        P(("tensor", "dp"), "ctx"),
        P(("tensor", "dp"), "ctx"),
        P("ctx"),
        P(("ctx", "dp"), "tensor"),
        P(("ctx", "dp"), "tensor"),
        P("tensor"),
        P(),
    )
    out_specs = (
        P(("tensor", "dp"), "ctx"),
        P(("tensor", "dp"), "ctx"),
        P("ctx"),
        P(("tensor", "dp"), "ctx"),
        P(("ctx", "dp"), "tensor"),
        P(("ctx", "dp"), "tensor"),
        P("tensor"),
        P(("ctx", "dp"), "tensor"),
    )

    return jax.shard_map(shards, mesh=mesh, in_specs=in_specs, out_specs=out_specs, check_vma=False)
```

```python
import jax
import jax.numpy as jnp
from jax import lax
from jax.experimental import pallas as pl
from jax.experimental.pallas import tpu as pltpu
from jax.sharding import PartitionSpec as P

D = 4608
HEAD_DIM = 128
FF = 18432

BETA_ONE = 0.9
BETA_TWO = 0.95
EPSILON = 1e-08
LEARN_RATE = 0.003
DECAY_RATE = 0.1

LANES = 128
ROW_BLOCKS = 6
GROUPS = {
    "forward0": (((0, 2),), ((0, 1), (1, 1))),
    "forward1": (((1, 2),), ((0, 3), (1, 3), (0, 2), (1, 2))),
    "keep": (((0, 1), (1, 3)), ()),
    "rest": (((0, 3), (1, 1), (0, 0), (1, 0)), ((0, 0), (1, 0))),
}
ANY = pl.BlockSpec(memory_space=pl.ANY)
HBM = pl.BlockSpec(memory_space=pltpu.HBM)
VMEM = pl.BlockSpec(memory_space=pltpu.VMEM)


PARAMS = pltpu.CompilerParams(vmem_limit_bytes=8 << 20)


def pairs(size, mask):
    return [(i, i ^ mask) for i in range(size)]


def far(x):
    return pltpu.with_memory_space_constraint(x, pltpu.HBM)


def near(x):
    return pltpu.with_memory_space_constraint(x, pltpu.VMEM)


def down_rows(width):
    return 2 * width + width // 4


def query_rows(query_chunks):
    return query_chunks.shape[1] * query_chunks.shape[2] // (2 * LANES)


def pack(parts, columns, query_chunks, after, place):
    q_rows, q_cols = query_chunks.shape[1:]
    q_wide = q_cols // LANES // 2
    width = columns.shape[0]
    quarter = width // 4
    block, query = down_rows(width), query_rows(query_chunks)
    span = columns.shape[1] // 4

    def kernel(down_ref, query_ref, _, *refs):
        outs, bufs, sems = refs[: len(parts)], refs[len(parts) : 2 * len(parts)], refs[2 * len(parts) :]
        me = lax.axis_index("dp")
        y, core = me // 2, me % 2
        shared, whole = [], []

        def put(copies, source, target, semaphore):
            if place is far:
                copies.append(pltpu.make_async_copy(source, target, semaphore))
            else:
                target[...] = source[...]

        for (group, mine), out, buf, sem in zip(parts, outs, bufs, sems):
            downs, queries = GROUPS[group]
            owner = core if mine else 1 - core
            for at, (half, d) in enumerate(downs):
                lane = pl.multiple_of(span * (y ^ d) + 4 * LANES, LANES)
                source = down_ref.at[pl.ds(half * 2 * quarter, 2 * quarter), pl.ds(lane, LANES)]
                put(shared, source, buf.at[at], sem.at[at, 0])
            for at, (half, d) in enumerate(downs):
                for j in range(2):
                    lane = pl.multiple_of(span * (y ^ d) + 5 * LANES * owner + (2 * half + j) * LANES, LANES)
                    target = out.at[pl.ds(at * block + j * (width + quarter), width), :]
                    put(whole, down_ref.at[:, pl.ds(lane, LANES)], target, sem.at[at, 1 + j])
            for at, (half, d) in enumerate(queries):
                for j in range(q_wide):
                    source = query_ref.at[2 * (y ^ d) + owner, :, pl.ds((half * q_wide + j) * LANES, LANES)]
                    target = out.at[pl.ds(len(downs) * block + at * query + j * q_rows, q_rows), :]
                    put(whole, source, target, sem.at[at, 3 + j])
        for copy in shared + whole:
            copy.start()
        for copy in shared:
            copy.wait()
        low = lax.broadcasted_iota(jnp.int32, (quarter, LANES), 1) < LANES // 2
        for (group, mine), out, buf in zip(parts, outs, bufs):
            lower = (core == 0) if mine else (core == 1)
            for at in range(len(GROUPS[group][0])):
                first = buf[at, :quarter, :].astype(jnp.float32)
                second = buf[at, quarter:, :].astype(jnp.float32)
                packed = jnp.where(
                    lower,
                    jnp.where(low, first, pltpu.roll(second, LANES // 2, 1)),
                    jnp.where(low, pltpu.roll(first, LANES // 2, 1), second),
                )
                out[pl.ds(at * block + width, quarter), :] = packed.astype(jnp.bfloat16)
        for copy in whole:
            copy.wait()

    def rows(group):
        downs, queries = GROUPS[group]
        return len(downs) * block + len(queries) * query

    return pl.pallas_call(
        kernel,
        out_shape=tuple(pltpu.VMEM((rows(group), LANES), jnp.bfloat16) for group, _ in parts),
        in_specs=[HBM, HBM, ANY] if place is far else [VMEM, VMEM, ANY],
        out_specs=(VMEM,) * len(parts),
        scratch_shapes=[pltpu.VMEM((len(GROUPS[group][0]), 2 * quarter, LANES), jnp.bfloat16) for group, _ in parts]
        + [pltpu.SemaphoreType.DMA((4, 5)) for _ in parts],
        compiler_params=PARAMS,
    )(place(columns), place(query_chunks), after)


def added(*terms):
    total = terms[0].astype(jnp.float32)
    for term in terms[1:]:
        total = total + term.astype(jnp.float32)
    return total


def sent(x, mask, axis="dp"):
    return lax.ppermute(x, axis, pairs(8, mask))


def summed(*terms):
    return added(*terms).astype(jnp.bfloat16)


def moment_new(before, grad):
    return BETA_ONE * before + (1.0 - BETA_ONE) * grad


def column_sum(x):
    return jnp.sum(x * x, axis=0, keepdims=True)


def gather_query(query, own, other, direct, query_moment):
    q_rows, q_cols = query_moment.shape
    q_wide = q_cols // LANES // 2

    def kernel(own_ref, other_ref, from_first, from_second, from_third, moment_ref, new_ref, sums_ref):
        sums_ref[...] = jnp.zeros_like(sums_ref)
        for half in range(2):
            for j in range(q_wide):
                terms = []
                for ref in (own_ref, other_ref, from_first, from_second, from_third):
                    at = ref.shape[0] - (2 - half) * query + j * q_rows
                    terms.append(ref[pl.ds(at, q_rows), :])
                grad = added(*terms) * (1.0 / 8.0)
                head = half * q_wide + j
                span = (slice(None), slice(head * LANES, (head + 1) * LANES))
                new_ref[span] = moment_new(moment_ref[span], grad)
                sums_ref[head : head + 1, :] = column_sum(grad)

    return pl.pallas_call(
        kernel,
        out_shape=(pltpu.VMEM(query_moment.shape, jnp.float32), pltpu.VMEM((8, LANES), jnp.float32)),
        in_specs=[VMEM] * 6,
        out_specs=(VMEM,) * 2,
        compiler_params=PARAMS,
        name="query",
    )(*(near(t) for t in (own, other, *direct, query_moment)))


def gather(own, other, keeps, seconds, heads, down_moment):
    _, width = down_moment.shape
    quarter = width // 4
    block = down_rows(width)
    half_tile = LANES // 2
    tensors = lax.axis_size("tensor")

    def kernel(own_ref, other_ref, keep0, keep1, second0, second1, heads_ref, moment_ref, new_ref, message_ref):
        core = lax.axis_index("dp") % 2
        me = lax.axis_index("tensor")

        def mean(half, at, count):
            kept = (2 + half) * block + at
            return added(
                own_ref[pl.ds(kept, count), :],
                other_ref[pl.ds(kept, count), :],
                (keep0, keep1)[half][pl.ds(at, count), :],
                (second0, second1)[half][pl.ds(at, count), :],
            ) * (1.0 / 8.0)

        parts = []
        for half in range(2):
            packed = mean(half, width, quarter)
            parts += [packed, pltpu.roll(packed, half_tile, 1)]
        rest = jnp.concatenate(parts, axis=0)
        row = lax.broadcasted_iota(jnp.int32, (8, LANES), 0)
        lane = lax.broadcasted_iota(jnp.int32, (8, LANES), 1)
        neurons = jnp.zeros((8, LANES), jnp.float32)
        for c in range(0, width, LANES):
            step = min(LANES, width - c)
            span = slice(c, c + step)
            total = jnp.zeros((1, step), jnp.float32)
            for tile in range(4):
                grad = mean(tile // 2, (tile % 2) * (width + quarter) + c, step).T
                at = (pl.ds(pl.multiple_of(half_tile * core + tile * LANES, half_tile), LANES), span)
                new_ref[at] = moment_new(moment_ref[at], grad)
                total += column_sum(grad)
            grad = rest[c : c + step].T[:half_tile]
            at = (pl.ds(pl.multiple_of(4 * LANES * (1 - core), half_tile), half_tile), span)
            new_ref[at] = moment_new(moment_ref[at], grad)
            total += column_sum(grad)
            if step < LANES:
                total = jnp.pad(total, ((0, 0), (0, LANES - step)))
            neurons += jnp.where(row == c // LANES, total, 0.0)
        sums = jnp.sum(heads_ref[...], axis=1, keepdims=True)
        spread = jnp.sum(jnp.where(row == lane, sums, 0.0), axis=0, keepdims=True)
        mine = neurons + jnp.where(row == 5, spread, 0.0)
        for target in range(message_ref.shape[0]):
            message_ref[target] = jnp.where(me == target % tensors, mine, neurons)

    return pl.pallas_call(
        kernel,
        out_shape=(
            pltpu.VMEM(down_moment.shape, jnp.float32),
            pltpu.VMEM((lax.axis_size("dp") * tensors, 8, LANES), jnp.float32),
        ),
        in_specs=[VMEM] * 8,
        out_specs=(VMEM,) * 2,
        compiler_params=PARAMS,
        name="gather",
    )(*(near(t) for t in (own, other, *keeps, *seconds, heads, down_moment)))


def store_kernel(new_ref, query_new_ref, moment_out, query_moment_out, sems):
    copies = (
        pltpu.make_async_copy(new_ref, moment_out, sems.at[0]),
        pltpu.make_async_copy(query_new_ref, query_moment_out, sems.at[1]),
    )
    for copy in copies:
        copy.start()
    for copy in copies:
        copy.wait()


def finish_kernel(
    keep_ref, got_ref, new_ref, param_ref, second_ref, query_new_ref, query_param_ref, query_second_ref,
    param_out, update_out, second_out, query_param_out, query_update_out, query_second_out,
    param_buf, update_buf, second_buf, query_param_buf, query_update_buf, query_second_buf, sems, query_sems, second_sems,
):
    keep_one, keep_two = keep_ref[:, 0:1], keep_ref[:, 1:2]
    total = jnp.sum(got_ref[...], axis=0)

    def second_new(before, mean):
        return BETA_TWO * before + (1.0 - BETA_TWO) * mean

    def factor(second):
        return 1.0 / (keep_one * (jnp.sqrt(second / keep_two) + EPSILON))

    def write(at, scale, new, param, update_to, param_to):
        old = param[at]
        update = new[at] * scale
        update_to[at] = update.astype(jnp.bfloat16)
        param_to[at] = old - LEARN_RATE * (update + DECAY_RATE * old)

    rows, cols = new_ref.shape
    spans = [slice(k, min(k + LANES, cols)) for k in range(0, cols, LANES)]
    factors = []
    for k, span in enumerate(spans):
        second = second_new(second_ref[:, span], total[k : k + 1, : span.stop - span.start] * (1.0 / FF))
        second_buf[span] = second[0]
        factors.append(factor(second))
    copies = [pltpu.make_async_copy(second_buf, second_out, second_sems.at[0])]
    copies[-1].start()
    block = rows // ROW_BLOCKS
    for b in range(ROW_BLOCKS):
        part = slice(b * block, (b + 1) * block)
        for span, scale in zip(spans, factors):
            write((part, span), scale, new_ref, param_ref, update_buf, param_buf)
        copies.append(pltpu.make_async_copy(param_buf.at[part], param_out.at[part], sems.at[0, b]))
        copies.append(pltpu.make_async_copy(update_buf.at[part], update_out.at[part], sems.at[1, b]))
        copies[-2].start()
        copies[-1].start()
    heads = query_new_ref.shape[1] // HEAD_DIM
    for head in range(heads):
        mean = total[5:6, head : head + 1] * (1.0 / (D * HEAD_DIM))
        second = second_new(query_second_ref[:, head : head + 1], mean)
        query_second_buf[:, head : head + 1] = second
        span = slice(head * HEAD_DIM, (head + 1) * HEAD_DIM)
        write((slice(None), span), factor(second), query_new_ref, query_param_ref, query_update_buf, query_param_buf)
    copies.append(pltpu.make_async_copy(query_param_buf, query_param_out, query_sems.at[0]))
    copies.append(pltpu.make_async_copy(query_update_buf, query_update_out, query_sems.at[1]))
    copies.append(pltpu.make_async_copy(query_second_buf, query_second_out, second_sems.at[1]))
    for copy in copies[-3:]:
        copy.start()
    for copy in copies:
        copy.wait()


def shards(
    grad_down,
    grad_query,
    down_param,
    down_moment,
    down_second,
    query_param,
    query_moment,
    query_second,
    step_count,
):
    replicas = lax.axis_size("dp")
    step_value = step_count[0].astype(jnp.float32)
    keep = jnp.stack(
        [1.0 - jnp.power(jnp.float32(BETA_ONE), step_value), 1.0 - jnp.power(jnp.float32(BETA_TWO), step_value)]
    )
    columns = grad_down[0].T
    query_chunks = grad_query[0].reshape(replicas, -1, grad_query.shape[2])
    width = columns.shape[0]
    block, query = down_rows(width), query_rows(query_chunks)

    def packed(after, place, *parts):
        return pack(parts, columns, query_chunks, after, place)

    def other_core(x):
        return sent(x, 1)

    to_first, to_second = (2, 6), (6, 2)
    sends = packed(query_chunks, far, ("forward0", False), ("forward1", False))
    others = [other_core(sends[half]) for half in range(2)]
    owns = packed(sends[0], near, ("forward0", True), ("forward1", True))
    ends = [block + 2 * query] * 2
    forwards = [summed(owns[half][: ends[half]], others[half][: ends[half]]) for half in range(2)]
    across = summed(owns[1][ends[1] :], others[1][ends[1] :])
    forwards = [sent(forwards[half], to_first[half]) for half in range(2)]
    across = sent(across, 4)
    keep_send, keep_own = packed(owns[0], near, ("keep", False), ("keep", True))
    keep_other = other_core(keep_send)
    send, own = packed(keep_own, near, ("rest", False), ("rest", True))
    other = other_core(send)
    keeps = []
    for half in range(2):
        part = slice(half * block, (half + 1) * block)
        keeps.append(summed(keep_own[part], keep_other[part]))
    keeps = [sent(keeps[half], to_first[half]) for half in range(2)]
    seconds = []
    for half in range(2):
        part = slice(half * block, (half + 1) * block)
        seconds.append(summed(own[part], other[part], forwards[half][:block]))
    seconds = [sent(seconds[half], to_second[half]) for half in range(2)]
    query_new, heads = gather_query(query, own, other, (*forwards, across), query_moment)
    for mask in (1, 2, 7):
        heads = heads + sent(heads, mask, "ctx")
    new, message = gather(own, other, keeps, seconds, heads, down_moment)
    got = lax.all_to_all(message, ("dp", "tensor"), split_axis=0, concat_axis=0, tiled=True)
    down_moment_new, query_moment_new = pl.pallas_call(
        store_kernel,
        out_shape=tuple(pltpu.HBM(x.shape, jnp.float32) for x in (new, query_new)),
        in_specs=[VMEM, VMEM],
        out_specs=(HBM, HBM),
        scratch_shapes=[pltpu.SemaphoreType.DMA((2,))],
        compiler_params=PARAMS,
        name="store",
    )(near(new), near(query_new))
    f32, bf16 = jnp.float32, jnp.bfloat16
    outs = pl.pallas_call(
        finish_kernel,
        out_shape=(
            pltpu.HBM(down_param.shape, f32),
            pltpu.HBM(down_param.shape, bf16),
            pltpu.HBM(down_second.shape, f32),
            pltpu.HBM(query_param.shape, f32),
            pltpu.HBM(query_param.shape, bf16),
            pltpu.HBM((1, query_second.shape[0]), f32),
        ),
        in_specs=[VMEM] * 8,
        out_specs=(HBM,) * 6,
        scratch_shapes=[
            pltpu.VMEM(down_param.shape, f32),
            pltpu.VMEM(down_param.shape, bf16),
            pltpu.VMEM(down_second.shape, f32),
            pltpu.VMEM(query_param.shape, f32),
            pltpu.VMEM(query_param.shape, bf16),
            pltpu.VMEM((1, query_second.shape[0]), f32),
            pltpu.SemaphoreType.DMA((2, ROW_BLOCKS)),
            pltpu.SemaphoreType.DMA((2,)),
            pltpu.SemaphoreType.DMA((2,)),
        ],
        compiler_params=PARAMS, name="finish",
    )(
        near(keep[None, :]), near(got), near(new), near(down_param), near(down_second[None, :]),
        near(query_new), near(query_param), near(query_second[None, :]),
    )
    down_param_new, down_update, down_second_new = outs[:3]
    query_param_new, query_update, query_second_new = outs[3:]
    return (
        down_param_new,
        down_moment_new,
        down_second_new,
        down_update,
        query_param_new,
        query_moment_new,
        query_second_new[0],
        query_update,
    )


def solution(mesh):
    in_specs = (
        P("dp", "tensor", "ctx"),
        P("dp", "ctx", "tensor"),
        P(("tensor", "dp"), "ctx"),
        P(("tensor", "dp"), "ctx"),
        P("ctx"),
        P(("ctx", "dp"), "tensor"),
        P(("ctx", "dp"), "tensor"),
        P("tensor"),
        P(),
    )
    out_specs = (
        P(("tensor", "dp"), "ctx"),
        P(("tensor", "dp"), "ctx"),
        P("ctx"),
        P(("tensor", "dp"), "ctx"),
        P(("ctx", "dp"), "tensor"),
        P(("ctx", "dp"), "tensor"),
        P("tensor"),
        P(("ctx", "dp"), "tensor"),
    )

    return jax.shard_map(shards, mesh=mesh, in_specs=in_specs, out_specs=out_specs, check_vma=False)
```

```python
import jax
import jax.numpy as jnp
from jax import lax
from jax.experimental import pallas as pl
from jax.experimental.pallas import tpu as pltpu
from jax.sharding import PartitionSpec as P

D = 4608
HEAD_DIM = 128
FF = 18432

BETA_ONE = 0.9
BETA_TWO = 0.95
EPSILON = 1e-08
LEARN_RATE = 0.003
DECAY_RATE = 0.1

LANES = 128
ROW_BLOCKS = 6
GROUPS = {
    "query": ((), ((0, 2), (0, 1), (1, 2), (1, 3), (0, 3), (1, 1), (0, 0), (1, 0))),
    "forward0": (((0, 2),), ()),
    "forward1": (((1, 2),), ()),
    "keep": (((0, 1), (1, 3)), ()),
    "rest": (((0, 3), (1, 1), (0, 0), (1, 0)), ()),
}
ANY = pl.BlockSpec(memory_space=pl.ANY)
HBM = pl.BlockSpec(memory_space=pltpu.HBM)
VMEM = pl.BlockSpec(memory_space=pltpu.VMEM)


PARAMS = pltpu.CompilerParams(vmem_limit_bytes=8 << 20)


def pairs(size, mask):
    return [(i, i ^ mask) for i in range(size)]


def far(x):
    return pltpu.with_memory_space_constraint(x, pltpu.HBM)


def near(x):
    return pltpu.with_memory_space_constraint(x, pltpu.VMEM)


def down_rows(width):
    return 2 * width + width // 4


def query_rows(query_chunks):
    return query_chunks.shape[1] * query_chunks.shape[2] // (2 * LANES)


def pack(parts, columns, query_chunks, after, place):
    q_rows, q_cols = query_chunks.shape[1:]
    q_wide = q_cols // LANES // 2
    width = columns.shape[0]
    quarter = width // 4
    block, query = down_rows(width), query_rows(query_chunks)
    span = columns.shape[1] // 4

    def kernel(down_ref, query_ref, _, *refs):
        outs, bufs, sems = (refs[i * len(parts) : (i + 1) * len(parts)] for i in range(3))
        query_buf, query_sem = refs[3 * len(parts) :]
        me = lax.axis_index("dp")
        y, core = me // 2, me % 2
        shared, whole, moves, chunks = [], [], [], {}

        def put(copies, source, target, semaphore):
            if place is far:
                copies.append(pltpu.make_async_copy(source, target, semaphore))
            else:
                target[...] = source[...]

        for (group, mine), out, buf, sem in zip(parts, outs, bufs, sems):
            downs, queries = GROUPS[group]
            owner = core if mine else 1 - core
            for at, (half, d) in enumerate(downs):
                lane = pl.multiple_of(span * (y ^ d) + 4 * LANES, LANES)
                source = down_ref.at[pl.ds(half * 2 * quarter, 2 * quarter), pl.ds(lane, LANES)]
                put(shared, source, buf.at[at], sem.at[0, 0])
            for at, (half, d) in enumerate(downs):
                for j in range(2):
                    lane = pl.multiple_of(span * (y ^ d) + 5 * LANES * owner + (2 * half + j) * LANES, LANES)
                    target = out.at[pl.ds(at * block + j * (width + quarter), width), :]
                    put(whole, down_ref.at[:, pl.ds(lane, LANES)], target, sem.at[0, 1 + j])
            for at, (half, d) in enumerate(queries):
                chunk = query_ref.at[2 * (y ^ d) + owner]
                if place is far:
                    chunk = query_buf.at[0, d]
                    chunks[d] = pltpu.make_async_copy(
                        query_ref.at[2 * (y ^ d) + owner], chunk, query_sem.at[0, d]
                    )
                for j in range(q_wide):
                    source = chunk.at[:, pl.ds((half * q_wide + j) * LANES, LANES)]
                    target = out.at[pl.ds(len(downs) * block + at * query + j * q_rows, q_rows), :]
                    if place is far:
                        moves.append((source, target))
                    else:
                        target[...] = source[...]
        for copy in (*chunks.values(), *shared, *whole):
            copy.start()
        for copy in (*chunks.values(), *shared):
            copy.wait()
        for source, target in moves:
            target[...] = source[...]
        low = lax.broadcasted_iota(jnp.int32, (quarter, LANES), 1) < LANES // 2
        for (group, mine), out, buf in zip(parts, outs, bufs):
            lower = (core == 0) if mine else (core == 1)
            for at in range(len(GROUPS[group][0])):
                first = buf[at, :quarter, :].astype(jnp.float32)
                second = buf[at, quarter:, :].astype(jnp.float32)
                packed = jnp.where(
                    lower,
                    jnp.where(low, first, pltpu.roll(second, LANES // 2, 1)),
                    jnp.where(low, pltpu.roll(first, LANES // 2, 1), second),
                )
                out[pl.ds(at * block + width, quarter), :] = packed.astype(jnp.bfloat16)
        for copy in whole:
            copy.wait()

    def rows(group):
        downs, queries = GROUPS[group]
        return len(downs) * block + len(queries) * query

    return pl.pallas_call(
        kernel,
        out_shape=tuple(pltpu.VMEM((rows(group), LANES), jnp.bfloat16) for group, _ in parts),
        in_specs=[HBM, HBM, ANY] if place is far else [VMEM, VMEM, ANY],
        out_specs=(VMEM,) * len(parts),
        scratch_shapes=[
            pltpu.VMEM((max(len(GROUPS[group][0]), 1), 2 * quarter, LANES), jnp.bfloat16) for group, _ in parts
        ]
        + [pltpu.SemaphoreType.DMA((1, 3)) for _ in parts]
        + [pltpu.VMEM((1, 4, q_rows, q_cols), jnp.bfloat16), pltpu.SemaphoreType.DMA((1, 4))],
        compiler_params=PARAMS,
    )(place(columns), place(query_chunks), after)


def added(*terms):
    total = terms[0].astype(jnp.float32)
    for term in terms[1:]:
        total = total + term.astype(jnp.float32)
    return total


def sent(x, mask, axis="dp"):
    return lax.ppermute(x, axis, pairs(8, mask))


def summed(*terms):
    return added(*terms).astype(jnp.bfloat16)


def moment_new(before, grad):
    return BETA_ONE * before + (1.0 - BETA_ONE) * grad


def column_sum(x):
    return jnp.sum(x * x, axis=0, keepdims=True)


def gather_query(query, own, other, asks, asked, query_moment):
    q_rows, q_cols = query_moment.shape
    q_wide = q_cols // LANES // 2

    def kernel(own_ref, other_ref, ask0, ask1, asked0, asked1, moment_ref, new_ref, sums_ref):
        sums_ref[...] = jnp.zeros_like(sums_ref)
        for half in range(2):
            for j in range(q_wide):
                kept, at = (6 + half) * query + j * q_rows, j * q_rows
                grad = added(
                    own_ref[pl.ds(kept, q_rows), :],
                    other_ref[pl.ds(kept, q_rows), :],
                    (ask0, ask1)[half][pl.ds(query + at, q_rows), :],
                    (asked0, asked1)[half][pl.ds(at, q_rows), :],
                ) * (1.0 / 8.0)
                head = half * q_wide + j
                span = (slice(None), slice(head * LANES, (head + 1) * LANES))
                new_ref[span] = moment_new(moment_ref[span], grad)
                sums_ref[head : head + 1, :] = column_sum(grad)

    return pl.pallas_call(
        kernel,
        out_shape=(pltpu.VMEM(query_moment.shape, jnp.float32), pltpu.VMEM((8, LANES), jnp.float32)),
        in_specs=[VMEM] * 7,
        out_specs=(VMEM,) * 2,
        compiler_params=PARAMS,
        name="query",
    )(*(near(t) for t in (own, other, *asks, *asked, query_moment)))


def gather(own, other, keeps, seconds, heads, down_moment):
    _, width = down_moment.shape
    quarter = width // 4
    block = down_rows(width)
    half_tile = LANES // 2
    tensors = lax.axis_size("tensor")

    def kernel(own_ref, other_ref, keep0, keep1, second0, second1, heads_ref, moment_ref, new_ref, message_ref):
        core = lax.axis_index("dp") % 2
        me = lax.axis_index("tensor")

        def mean(half, at, count):
            kept = (2 + half) * block + at
            return added(
                own_ref[pl.ds(kept, count), :],
                other_ref[pl.ds(kept, count), :],
                (keep0, keep1)[half][pl.ds(at, count), :],
                (second0, second1)[half][pl.ds(at, count), :],
            ) * (1.0 / 8.0)

        parts = []
        for half in range(2):
            packed = mean(half, width, quarter)
            parts += [packed, pltpu.roll(packed, half_tile, 1)]
        rest = jnp.concatenate(parts, axis=0)
        row = lax.broadcasted_iota(jnp.int32, (8, LANES), 0)
        lane = lax.broadcasted_iota(jnp.int32, (8, LANES), 1)
        neurons = jnp.zeros((8, LANES), jnp.float32)
        for c in range(0, width, LANES):
            step = min(LANES, width - c)
            span = slice(c, c + step)
            total = jnp.zeros((1, step), jnp.float32)
            for tile in range(4):
                grad = mean(tile // 2, (tile % 2) * (width + quarter) + c, step).T
                at = (pl.ds(pl.multiple_of(half_tile * core + tile * LANES, half_tile), LANES), span)
                new_ref[at] = moment_new(moment_ref[at], grad)
                total += column_sum(grad)
            grad = rest[c : c + step].T[:half_tile]
            at = (pl.ds(pl.multiple_of(4 * LANES * (1 - core), half_tile), half_tile), span)
            new_ref[at] = moment_new(moment_ref[at], grad)
            total += column_sum(grad)
            if step < LANES:
                total = jnp.pad(total, ((0, 0), (0, LANES - step)))
            neurons += jnp.where(row == c // LANES, total, 0.0)
        sums = jnp.sum(heads_ref[...], axis=1, keepdims=True)
        spread = jnp.sum(jnp.where(row == lane, sums, 0.0), axis=0, keepdims=True)
        mine = neurons + jnp.where(row == 5, spread, 0.0)
        for target in range(message_ref.shape[0]):
            message_ref[target] = jnp.where(me == target % tensors, mine, neurons)

    return pl.pallas_call(
        kernel,
        out_shape=(
            pltpu.VMEM(down_moment.shape, jnp.float32),
            pltpu.VMEM((lax.axis_size("dp") * tensors, 8, LANES), jnp.float32),
        ),
        in_specs=[VMEM] * 8,
        out_specs=(VMEM,) * 2,
        compiler_params=PARAMS,
        name="gather",
    )(*(near(t) for t in (own, other, *keeps, *seconds, heads, down_moment)))


def store_kernel(new_ref, query_new_ref, moment_out, query_moment_out, sems):
    copies = (
        pltpu.make_async_copy(new_ref, moment_out, sems.at[0]),
        pltpu.make_async_copy(query_new_ref, query_moment_out, sems.at[1]),
    )
    for copy in copies:
        copy.start()
    for copy in copies:
        copy.wait()


def finish_kernel(
    keep_ref, got_ref, new_ref, param_ref, second_ref, query_new_ref, query_param_ref, query_second_ref,
    param_out, update_out, second_out, query_param_out, query_update_out, query_second_out,
    param_buf, update_buf, second_buf, query_param_buf, query_update_buf, query_second_buf, sems, query_sems, second_sems,
):
    keep_one, keep_two = keep_ref[:, 0:1], keep_ref[:, 1:2]
    total = jnp.sum(got_ref[...], axis=0)

    def second_new(before, mean):
        return BETA_TWO * before + (1.0 - BETA_TWO) * mean

    def factor(second):
        return 1.0 / (keep_one * (jnp.sqrt(second / keep_two) + EPSILON))

    def write(at, scale, new, param, update_to, param_to):
        old = param[at]
        update = new[at] * scale
        update_to[at] = update.astype(jnp.bfloat16)
        param_to[at] = old - LEARN_RATE * (update + DECAY_RATE * old)

    rows, cols = new_ref.shape
    spans = [slice(k, min(k + LANES, cols)) for k in range(0, cols, LANES)]
    factors = []
    for k, span in enumerate(spans):
        second = second_new(second_ref[:, span], total[k : k + 1, : span.stop - span.start] * (1.0 / FF))
        second_buf[span] = second[0]
        factors.append(factor(second))
    copies = [pltpu.make_async_copy(second_buf, second_out, second_sems.at[0])]
    copies[-1].start()
    block = rows // ROW_BLOCKS
    for b in range(ROW_BLOCKS):
        part = slice(b * block, (b + 1) * block)
        for span, scale in zip(spans, factors):
            write((part, span), scale, new_ref, param_ref, update_buf, param_buf)
        copies.append(pltpu.make_async_copy(param_buf.at[part], param_out.at[part], sems.at[0, b]))
        copies.append(pltpu.make_async_copy(update_buf.at[part], update_out.at[part], sems.at[1, b]))
        copies[-2].start()
        copies[-1].start()
    heads = query_new_ref.shape[1] // HEAD_DIM
    for head in range(heads):
        mean = total[5:6, head : head + 1] * (1.0 / (D * HEAD_DIM))
        second = second_new(query_second_ref[:, head : head + 1], mean)
        query_second_buf[:, head : head + 1] = second
        span = slice(head * HEAD_DIM, (head + 1) * HEAD_DIM)
        write((slice(None), span), factor(second), query_new_ref, query_param_ref, query_update_buf, query_param_buf)
    copies.append(pltpu.make_async_copy(query_param_buf, query_param_out, query_sems.at[0]))
    copies.append(pltpu.make_async_copy(query_update_buf, query_update_out, query_sems.at[1]))
    copies.append(pltpu.make_async_copy(query_second_buf, query_second_out, second_sems.at[1]))
    for copy in copies[-3:]:
        copy.start()
    for copy in copies:
        copy.wait()


def shards(
    grad_down,
    grad_query,
    down_param,
    down_moment,
    down_second,
    query_param,
    query_moment,
    query_second,
    step_count,
):
    replicas = lax.axis_size("dp")
    step_value = step_count[0].astype(jnp.float32)
    keep = jnp.stack(
        [1.0 - jnp.power(jnp.float32(BETA_ONE), step_value), 1.0 - jnp.power(jnp.float32(BETA_TWO), step_value)]
    )
    columns = grad_down[0].T
    query_chunks = grad_query[0].reshape(replicas, -1, grad_query.shape[2])
    width = columns.shape[0]
    block, query = down_rows(width), query_rows(query_chunks)

    def packed(after, place, *parts):
        return pack(parts, columns, query_chunks, after, place)

    def other_core(x):
        return sent(x, 1)

    to_first, to_second = (2, 6), (6, 2)
    send_query, *sends = packed(query_chunks, far, ("query", False), ("forward0", False), ("forward1", False))
    other_query = other_core(send_query)
    others = [other_core(sends[half]) for half in range(2)]
    own_query, *owns = packed(send_query, near, ("query", True), ("forward0", True), ("forward1", True))
    asks = []
    for half in range(2):
        part = slice(2 * half * query, 2 * (half + 1) * query)
        asks.append(summed(own_query[part], other_query[part]))
    asks = [sent(asks[half], to_first[half]) for half in range(2)]
    forwards = [summed(owns[half], others[half]) for half in range(2)]
    forwards = [sent(forwards[half], to_first[half]) for half in range(2)]
    asked = []
    for half in range(2):
        part = slice((4 + half) * query, (5 + half) * query)
        asked.append(summed(own_query[part], other_query[part], asks[half][:query]))
    asked = [sent(asked[half], to_second[half]) for half in range(2)]
    keep_send, keep_own = packed(owns[0], near, ("keep", False), ("keep", True))
    keep_other = other_core(keep_send)
    send, own = packed(keep_own, near, ("rest", False), ("rest", True))
    other = other_core(send)
    keeps = []
    for half in range(2):
        part = slice(half * block, (half + 1) * block)
        keeps.append(summed(keep_own[part], keep_other[part]))
    keeps = [sent(keeps[half], to_first[half]) for half in range(2)]
    seconds = []
    for half in range(2):
        part = slice(half * block, (half + 1) * block)
        seconds.append(summed(own[part], other[part], forwards[half]))
    seconds = [sent(seconds[half], to_second[half]) for half in range(2)]
    query_new, heads = gather_query(query, own_query, other_query, asks, asked, query_moment)
    for mask in (1, 2, 7):
        heads = heads + sent(heads, mask, "ctx")
    new, message = gather(own, other, keeps, seconds, heads, down_moment)
    got = lax.all_to_all(message, ("dp", "tensor"), split_axis=0, concat_axis=0, tiled=True)
    down_moment_new, query_moment_new = pl.pallas_call(
        store_kernel,
        out_shape=tuple(pltpu.HBM(x.shape, jnp.float32) for x in (new, query_new)),
        in_specs=[VMEM, VMEM],
        out_specs=(HBM, HBM),
        scratch_shapes=[pltpu.SemaphoreType.DMA((2,))],
        compiler_params=PARAMS,
        name="store",
    )(near(new), near(query_new))
    f32, bf16 = jnp.float32, jnp.bfloat16
    outs = pl.pallas_call(
        finish_kernel,
        out_shape=(
            pltpu.HBM(down_param.shape, f32),
            pltpu.HBM(down_param.shape, bf16),
            pltpu.HBM(down_second.shape, f32),
            pltpu.HBM(query_param.shape, f32),
            pltpu.HBM(query_param.shape, bf16),
            pltpu.HBM((1, query_second.shape[0]), f32),
        ),
        in_specs=[VMEM] * 8,
        out_specs=(HBM,) * 6,
        scratch_shapes=[
            pltpu.VMEM(down_param.shape, f32),
            pltpu.VMEM(down_param.shape, bf16),
            pltpu.VMEM(down_second.shape, f32),
            pltpu.VMEM(query_param.shape, f32),
            pltpu.VMEM(query_param.shape, bf16),
            pltpu.VMEM((1, query_second.shape[0]), f32),
            pltpu.SemaphoreType.DMA((2, ROW_BLOCKS)),
            pltpu.SemaphoreType.DMA((2,)),
            pltpu.SemaphoreType.DMA((2,)),
        ],
        compiler_params=PARAMS, name="finish",
    )(
        near(keep[None, :]), near(got), near(new), near(down_param), near(down_second[None, :]),
        near(query_new), near(query_param), near(query_second[None, :]),
    )
    down_param_new, down_update, down_second_new = outs[:3]
    query_param_new, query_update, query_second_new = outs[3:]
    return (
        down_param_new,
        down_moment_new,
        down_second_new,
        down_update,
        query_param_new,
        query_moment_new,
        query_second_new[0],
        query_update,
    )


def solution(mesh):
    in_specs = (
        P("dp", "tensor", "ctx"),
        P("dp", "ctx", "tensor"),
        P(("tensor", "dp"), "ctx"),
        P(("tensor", "dp"), "ctx"),
        P("ctx"),
        P(("ctx", "dp"), "tensor"),
        P(("ctx", "dp"), "tensor"),
        P("tensor"),
        P(),
    )
    out_specs = (
        P(("tensor", "dp"), "ctx"),
        P(("tensor", "dp"), "ctx"),
        P("ctx"),
        P(("tensor", "dp"), "ctx"),
        P(("ctx", "dp"), "tensor"),
        P(("ctx", "dp"), "tensor"),
        P("tensor"),
        P(("ctx", "dp"), "tensor"),
    )

    return jax.shard_map(shards, mesh=mesh, in_specs=in_specs, out_specs=out_specs, check_vma=False)
```
